512 devices in a mesh: row: 16 (over z, core), col: 32 (over y, x).
Axes of the slice: x: 4, y: 8, z: 8, core: 2. Of those that a mesh axis runs over, the one named last changes fastest.
Arguments:
- data: bfloat16 [32768, 32768], P('row', 'col'), may hold values from 0 to 30
- w_rows: bfloat16 [64, 32768], P(None, 'row'), may hold values from 0 to 1
- h_init: float32 [64, 32768], P(None, 'col'), may hold values from 0 to 0.4
Outputs:
- h_scaled: bfloat16 [64, 32768], P(None, 'col')
- h_gram: float32 [64, 64], replicated
- w_terms: float32 [64, 32768], P(None, ('row', 'col'))
The draws below stay inside these ranges and needn't reach their ends.
All inputs are finite; a program needn't handle non-finite values.
Results may differ from the reference program's by a relative error of at most 0.0005.
Values may be sent and summed in bfloat16 or wider, within the bound.
No kernel may reach another device: no remote copies, remote signals or barrier semaphores. Data moves between devices by JAX's collectives and lax.ppermute only.
A program may use at most 64 MiB of HBM per device.

```python
import math
import jax
import jax.numpy as jnp
from jax import lax

RANK = 64
ROWS_DEV = 2048
ITERS = 4
COLUMNS = 32768
ROWS = 32768


def draw_data(key, part):
    first, second, third = jax.random.split(jax.random.fold_in(key, 11), 3)
    blocks = ROWS // ROWS_DEV
    row_scale = jnp.exp(jax.random.uniform(first, (ROWS, 1), jnp.float32) * math.log(10.0))
    rising = jnp.exp(jnp.arange(COLUMNS, dtype=jnp.float32) / COLUMNS * math.log(3.0))
    block_scale = jnp.exp(jax.random.uniform(second, (blocks, 1, COLUMNS), jnp.float32) * math.log(10.0))
    col_scale = jnp.broadcast_to(block_scale, (blocks, ROWS_DEV, COLUMNS)).reshape(ROWS, COLUMNS) * rising[None, :]
    base = jax.random.uniform(third, (ROWS, COLUMNS), jnp.float32)
    return (base * row_scale * col_scale / 10.0).astype(jnp.bfloat16)


def draw_w_rows(key, part):
    first = jax.random.fold_in(jax.random.fold_in(key, 23), 0)
    third = jax.random.fold_in(jax.random.fold_in(key, 23), 2)
    blocks = ROWS // ROWS_DEV
    values = jax.random.uniform(first, (RANK, ROWS), jnp.float32)
    values = values ** 8
    offset = jax.random.randint(third, (), 0, blocks)
    home = (jnp.arange(RANK, dtype=jnp.int32) + offset) % blocks
    block_of = jnp.arange(ROWS, dtype=jnp.int32) // ROWS_DEV
    weight = jnp.where(home[:, None] == block_of[None, :], 1.0, 0.15).astype(jnp.float32)
    values = values * weight
    return values.astype(jnp.bfloat16)


def shard_levels(own_key, dims, cuts, least, top_value):
    gain, own = 1.0, jax.random.fold_in(own_key, 6)
    for position, parts in cuts:
        draws = jnp.exp(jax.random.uniform(jax.random.fold_in(own, position), (parts,), jnp.float32, least / len(cuts), top_value / len(cuts)))
        gain = gain * jnp.repeat(draws, dims[position] // parts).reshape([-1 if axis == position else 1 for axis in range(len(dims))])
    return gain


def setup_inputs(seed: int = 0) -> dict:
    seeds = jax.random.split(jax.random.key(seed), 4)
    data = draw_data(jax.random.fold_in(seeds[3], 71), 0)
    w_rows = draw_w_rows(jax.random.fold_in(seeds[3], 71), 0)
    h_init = jnp.clip(0.4 * jax.random.uniform(seeds[2], (RANK, COLUMNS), jnp.float32) ** shard_levels(seeds[2], (RANK, COLUMNS), ((1, 32),), -0.2, 0.2), 0.0, 0.4)
    return dict(data=data, w_rows=w_rows, h_init=h_init)


def reference(data, w_rows, h_init):
    target = jnp.dot(w_rows, data, preferred_element_type=jnp.float32)
    gram = lax.dot_general(w_rows, w_rows, (((1,), (1,)), ((), ())), preferred_element_type=jnp.float32)
    lip = jnp.max(lax.optimization_barrier(jnp.sum(gram, axis=1)))
    factor = h_init
    ahead = h_init
    momentum = 1.0
    for step in range(ITERS):
        slope = jnp.dot(gram, ahead, precision=lax.Precision.HIGHEST) - target
        fresh = jnp.maximum(ahead - slope / lip, 0.0)
        following = (1.0 + math.sqrt(1.0 + 4.0 * momentum * momentum)) / 2.0
        ahead = fresh + (momentum - 1.0) / following * (fresh - factor)
        factor = fresh
        momentum = following
    mean_squares = lax.optimization_barrier(jnp.mean(factor * factor, axis=1, keepdims=True))
    h_scaled = (factor * lax.rsqrt(mean_squares + 1e-06)).astype(jnp.bfloat16)
    h_gram = lax.dot_general(h_scaled, h_scaled, (((1,), (1,)), ((), ())), preferred_element_type=jnp.float32) / COLUMNS
    w_terms = lax.dot_general(h_scaled, data, (((1,), (1,)), ((), ())), preferred_element_type=jnp.float32) / COLUMNS
    return (h_scaled, h_gram, w_terms)
```

```python
import math

import jax
import jax.numpy as jnp
from jax import lax
from jax.experimental import pallas as pl
from jax.experimental.pallas import tpu as pltpu
from jax.sharding import PartitionSpec as P

ITERS = 4
LANES = 128
HALF = 64
MIB = 1 << 20


def low_lanes(x):
    return lax.broadcasted_iota(jnp.int32, x.shape, 1) < HALF


def turned(x):
    return pltpu.roll(x, HALF, 1)


def stack_sides(x):
    return jnp.where(low_lanes(x[:32]), x[:32], turned(x[32:]))


def stack_copies(x):
    return jnp.where(low_lanes(x[:32]), x[:32], x[32:])


def unstack(x):
    return jnp.concatenate([x, turned(x)], axis=0)


def halves_of_rank(spot_ref, w_ref, data_ref, h_ref, own_ref, send_ref, chunk_ref, acc, gacc):
    step = pl.program_id(0)

    @pl.when(step == 0)
    def _():
        acc[...] = jnp.zeros_like(acc)
        gacc[...] = jnp.zeros_like(gacc)
        start = h_ref[...]
        chunk_ref[...] = jnp.where(spot_ref[2] == 0, start, turned(start))

    w = w_ref[...]
    acc[...] += jnp.dot(w, data_ref[...], preferred_element_type=jnp.float32)
    gacc[...] += lax.dot_general(
        w, jnp.concatenate([w, w], axis=0), (((1,), (1,)), ((), ())), preferred_element_type=jnp.float32
    )

    @pl.when(step == pl.num_programs(0) - 1)
    def _():
        width = acc.shape[1] // 2
        first = spot_ref[0] == 0
        left = acc[:, :width]
        right = acc[:, width:]
        own_ref[:, :width] = jnp.where(first, left, right)
        send_ref[:, :width] = jnp.where(first, right, left)
        own_ref[:, width:] = gacc[...]
        send_ref[:, width:] = gacc[...]


def partial_products(spot, w_rows, data, h_init):
    rows, columns = data.shape
    rank = w_rows.shape[0]
    blocks = 4
    depth = rows // blocks
    out = jax.ShapeDtypeStruct((rank, columns // 2 + LANES), jnp.float32)
    whole = lambda i, spot: (0, 0)
    return pl.pallas_call(
        halves_of_rank,
        grid_spec=pltpu.PrefetchScalarGridSpec(
            num_scalar_prefetch=1,
            grid=(blocks,),
            in_specs=[
                pl.BlockSpec((rank, depth), lambda i, spot: (0, i)),
                pl.BlockSpec((depth, columns), lambda i, spot: (i, 0)),
                pl.BlockSpec((rank, LANES), lambda i, spot: (0, spot[1])),
            ],
            out_specs=[
                pl.BlockSpec(out.shape, whole),
                pl.BlockSpec(out.shape, whole),
                pl.BlockSpec((rank, LANES), whole),
            ],
            scratch_shapes=[pltpu.VMEM((rank, columns), jnp.float32), pltpu.VMEM((rank, LANES), jnp.float32)],
        ),
        out_shape=[out, out, jax.ShapeDtypeStruct((rank, LANES), jnp.float32)],
        compiler_params=pltpu.CompilerParams(vmem_limit_bytes=24 * MIB),
        name="products",
    )(spot, w_rows, data, h_init)


def packing(zs, own_ref, got_ref, out_ref):
    width = own_ref.shape[1] - LANES
    gram = stack_copies(own_ref[:, width:] + got_ref[:, width:])
    for tile in range(width // LANES):
        at = slice(tile * LANES, (tile + 1) * LANES)
        x = own_ref[:, at] + got_ref[:, at]
        top, low = x[:32], x[32:]
        left = low_lanes(top)
        for side, block in enumerate((jnp.where(left, top, turned(low)), jnp.where(left, turned(top), low))):
            base = (2 * tile + side) * 64
            out_ref[base : base + 32, :] = block
            out_ref[base + 32 : base + 64, :] = gram


def packed(zs, own, got):
    return pl.pallas_call(
        lambda *refs: packing(zs, *refs),
        out_shape=jax.ShapeDtypeStruct((zs * 64, LANES), jnp.float32),
        compiler_params=pltpu.CompilerParams(vmem_limit_bytes=8 * MIB),
        name="packing",
    )(own, got)


def iterating(zs, got_ref, start_ref, out_ref):
    total = got_ref[0:64, :]
    for part in range(1, zs):
        total = total + got_ref[part * 64 : part * 64 + 64, :]
    target = unstack(total[:32])
    gram = unstack(total[32:])[:, :HALF]
    lip = jnp.max(jnp.sum(gram, axis=1, keepdims=True))
    factor = start_ref[...]
    ahead = factor
    momentum = 1.0
    for step in range(ITERS):
        slope = jnp.dot(
            gram, ahead, precision=lax.Precision.HIGHEST, preferred_element_type=jnp.float32
        ) - target
        fresh = jnp.maximum(ahead - slope / lip, 0.0)
        following = (1.0 + math.sqrt(1.0 + 4.0 * momentum * momentum)) / 2.0
        ahead = fresh + (momentum - 1.0) / following * (fresh - factor)
        factor = fresh
        momentum = following
    block = stack_sides(factor)
    for part in range(zs):
        out_ref[part * 32 : part * 32 + 32, :] = block


def iterated(zs, got, start):
    return pl.pallas_call(
        lambda *refs: iterating(zs, *refs),
        out_shape=jax.ShapeDtypeStruct((zs * 32, LANES), jnp.float32),
        compiler_params=pltpu.CompilerParams(vmem_limit_bytes=8 * MIB),
        name="iterating",
    )(got, start)


def contracting(zs, spot_ref, own_ref, other_ref, data_ref, factor_ref, out_ref, lines, gram):
    step = pl.program_id(0)
    width = zs * HALF

    @pl.when(step == 0)
    def _():
        first = spot_ref[0] == 0
        for tile in range(zs // 2):
            a0, b0 = own_ref[tile * 64 : tile * 64 + 32, :], own_ref[tile * 64 + 32 : tile * 64 + 64, :]
            a1, b1 = other_ref[tile * 64 : tile * 64 + 32, :], other_ref[tile * 64 + 32 : tile * 64 + 64, :]
            for side in range(2):
                a = jnp.where(first, a0, a1) if side == 0 else jnp.where(first, a1, a0)
                b = jnp.where(first, b0, b1) if side == 0 else jnp.where(first, b1, b0)
                left = low_lanes(a)
                x = jnp.concatenate([jnp.where(left, a, turned(b)), jnp.where(left, turned(a), b)], axis=0)
                at = slice(side * width + tile * LANES, side * width + (tile + 1) * LANES)
                factor_ref[:, at] = x
                low = x.astype(jnp.bfloat16)
                lines[0:64, at] = low
                lines[64:128, at] = low
        factor = factor_ref[...]
        squares = jnp.sum(factor * factor, axis=1, keepdims=True)
        outer = lax.dot_general(
            lines[0:64, :], lines[...], (((1,), (1,)), ((), ())), preferred_element_type=jnp.float32
        )
        row = lax.broadcasted_iota(jnp.int32, outer.shape, 0)
        lane = lax.broadcasted_iota(jnp.int32, outer.shape, 1)
        gram[...] = stack_copies(jnp.where(row == lane % HALF, squares, outer))

    terms = lax.dot_general(
        data_ref[...], lines[...], (((1,), (1,)), ((), ())), preferred_element_type=jnp.float32
    )
    for part in range(terms.shape[0] // 64):
        out_ref[part * 64 : part * 64 + 32, :] = stack_copies(terms[part * 64 : part * 64 + 64])
        out_ref[part * 64 + 32 : part * 64 + 64, :] = gram[...]


def contracted(zs, spot, own, other, data):
    rows, columns = data.shape
    blocks = 4
    depth = rows // blocks
    whole = lambda i, spot: (0, 0)
    return pl.pallas_call(
        lambda *refs: contracting(zs, *refs),
        grid_spec=pltpu.PrefetchScalarGridSpec(
            num_scalar_prefetch=1,
            grid=(blocks,),
            in_specs=[
                pl.BlockSpec(own.shape, whole),
                pl.BlockSpec(own.shape, whole),
                pl.BlockSpec((depth, columns), lambda i, spot: (i, 0)),
            ],
            out_specs=[
                pl.BlockSpec((64, columns), whole),
                pl.BlockSpec((depth, LANES), lambda i, spot: (i, 0)),
            ],
            scratch_shapes=[pltpu.VMEM((LANES, columns), jnp.bfloat16), pltpu.VMEM((32, LANES), jnp.float32)],
        ),
        out_shape=[
            jax.ShapeDtypeStruct((64, columns), jnp.float32),
            jax.ShapeDtypeStruct((rows, LANES), jnp.float32),
        ],
        compiler_params=pltpu.CompilerParams(vmem_limit_bytes=24 * MIB),
        name="contracting",
    )(spot, own, other, data)


def finishing(count, columns, got_ref, factor_ref, scaled_ref, gram_ref, terms_ref):
    total = got_ref[0:64, :]
    for part in range(1, count):
        total = total + got_ref[part * 64 : part * 64 + 64, :]
    outer = unstack(total[32:])
    row = lax.broadcasted_iota(jnp.int32, outer.shape, 0)
    lane = lax.broadcasted_iota(jnp.int32, outer.shape, 1)
    diagonal = jnp.where(row == lane, outer, 0.0)

    def scale_of(squares):
        mean = squares / columns + 1e-06
        first = lax.rsqrt(mean)
        return first * (1.5 - 0.5 * mean * first * first)

    down = scale_of(jnp.sum(diagonal, axis=1, keepdims=True))
    across = scale_of(jnp.sum(diagonal, axis=0, keepdims=True))
    scaled_ref[...] = (factor_ref[...] * down).astype(jnp.bfloat16)
    gram_ref[...] = (outer * down * across / columns)[:, :HALF]
    terms = jnp.transpose(unstack(total[:32]))[:HALF, :]
    terms_ref[...] = terms * down / columns


def finished(count, columns, got, factor):
    return pl.pallas_call(
        lambda *refs: finishing(count, columns, *refs),
        out_shape=[
            jax.ShapeDtypeStruct(factor.shape, jnp.bfloat16),
            jax.ShapeDtypeStruct((64, 64), jnp.float32),
            jax.ShapeDtypeStruct((64, 64), jnp.float32),
        ],
        compiler_params=pltpu.CompilerParams(vmem_limit_bytes=8 * MIB),
        name="finishing",
    )(got, factor)


def shards(data, w_rows, h_init):
    rows = lax.axis_size("row")
    zs = rows // 2
    columns = data.shape[1] * lax.axis_size("col")
    me = lax.axis_index("row")
    core, level = me % 2, me // 2
    at = core * (data.shape[1] // 2) + level * HALF
    spot = jnp.stack([core, at // LANES, level % 2]).astype(jnp.int32)
    swap = [(2 * z + c, 2 * z + 1 - c) for z in range(zs) for c in range(2)]
    level_groups = [[2 * z + c for z in range(zs)] for c in range(2)]

    own, send, start = partial_products(spot, w_rows, data, h_init)
    got = lax.ppermute(send, "row", swap)
    parts = packed(zs, own, got)
    parts = lax.all_to_all(parts, "row", 0, 0, tiled=True, axis_index_groups=level_groups)
    copies = iterated(zs, parts, start)
    mine = lax.all_to_all(copies, "row", 0, 0, tiled=True, axis_index_groups=level_groups)
    other = lax.ppermute(mine, "row", swap)
    factor, terms = contracted(zs, spot, mine, other, data)
    sums = lax.all_to_all(terms, "col", 0, 0, tiled=True)
    return tuple(finished(lax.axis_size("col"), columns, sums, factor))


def solution(mesh):
    in_specs = (P("row", "col"), P(None, "row"), P(None, "col"))
    out_specs = (P(None, "col"), P(), P(None, ("row", "col")))
    return jax.shard_map(shards, mesh=mesh, in_specs=in_specs, out_specs=out_specs, check_vma=False)
```

```python
import math

import jax
import jax.numpy as jnp
from jax import lax
from jax.experimental import pallas as pl
from jax.experimental.pallas import tpu as pltpu
from jax.sharding import PartitionSpec as P

ITERS = 4
LOG2E = 1.4426950408889634
LANES = 128
HALF = 64
BLOCKS = 4
CHUNK = 56
MIB = 1 << 20


def low_lanes(x):
    return lax.broadcasted_iota(jnp.int32, x.shape, 1) < HALF


def turned(x):
    return pltpu.roll(x, HALF, 1)


def stack_sides(x):
    return jnp.where(low_lanes(x[:32]), x[:32], turned(x[32:]))


def stack_copies(x):
    return jnp.where(low_lanes(x[:32]), x[:32], x[32:])


def unstack(x):
    return jnp.concatenate([x, turned(x)], axis=0)


def multiplying(zs, w_hbm, data_hbm, h_hbm, own_ref, send_ref, start_ref, data_ref, w, h, acc, sems):
    rows, columns = data_ref.shape
    width = columns // 2
    depth = rows // BLOCKS
    me = lax.axis_index("row")
    core, level = lax.rem(me, 2), lax.div(me, 2)
    tile = core * (width // LANES) + lax.div(level, 2)
    copies = [
        pltpu.make_async_copy(w_hbm, w, sems.at[BLOCKS]),
        pltpu.make_async_copy(
            h_hbm.at[:, pl.ds(pl.multiple_of(tile * LANES, LANES), LANES)], h, sems.at[BLOCKS + 1]
        ),
    ]
    for block in range(BLOCKS):
        at = pl.ds(block * depth, depth)
        copies.append(pltpu.make_async_copy(data_hbm.at[at, :], data_ref.at[at, :], sems.at[block]))
    for copy in (copies[0], *copies[2:], copies[1]):
        copy.start()
    copies[0].wait()
    gram = lax.dot_general(
        w[...], jnp.concatenate([w[...], w[...]], axis=0), (((1,), (1,)), ((), ())), preferred_element_type=jnp.float32
    )
    own_ref[:, width:] = gram
    send_ref[:, width:] = gram
    for block in range(BLOCKS):
        copies[2 + block].wait()
        at = slice(block * depth, (block + 1) * depth)
        part = jnp.dot(w[:, at], data_ref[at, :], preferred_element_type=jnp.float32)
        if block == 0:
            acc[...] = part
        else:
            acc[...] += part
    first = core == 0
    left = acc[:, :width]
    right = acc[:, width:]
    own_ref[:, :width] = jnp.where(first, left, right)
    send_ref[:, :width] = jnp.where(first, right, left)
    copies[1].wait()
    begin = h[...]
    start_ref[...] = jnp.where(lax.rem(level, 2) == 0, begin, turned(begin))


def multiplied(zs, w_rows, data, h_init):
    rows, columns = data.shape
    rank = w_rows.shape[0]
    half = jax.ShapeDtypeStruct((rank, columns // 2 + LANES), jnp.float32)
    start = jax.ShapeDtypeStruct((rank, LANES), jnp.float32)
    return pl.pallas_call(
        lambda *refs: multiplying(zs, *refs),
        in_specs=[pl.BlockSpec(memory_space=pl.ANY)] * 3,
        out_specs=[pl.BlockSpec(memory_space=pltpu.VMEM)] * 3,
        out_shape=[half, half, start],
        scratch_shapes=[
            pltpu.VMEM(data.shape, data.dtype),
            pltpu.VMEM(w_rows.shape, w_rows.dtype),
            pltpu.VMEM((rank, LANES), jnp.float32),
            pltpu.VMEM((rank, columns), jnp.float32),
            pltpu.SemaphoreType.DMA((BLOCKS + 2,)),
        ],
        compiler_params=pltpu.CompilerParams(vmem_limit_bytes=56045568),
        name="multiplying",
    )(w_rows, data, h_init)


def packing(zs, own_ref, got_ref, out_ref):
    width = own_ref.shape[1] - LANES
    gram = stack_copies(own_ref[:, width:] + got_ref[:, width:])
    for tile in range(width // LANES):
        at = slice(tile * LANES, (tile + 1) * LANES)
        x = own_ref[:, at] + got_ref[:, at]
        top, low = x[:32], x[32:]
        left = low_lanes(top)
        for side, block in enumerate((jnp.where(left, top, turned(low)), jnp.where(left, turned(top), low))):
            base = (2 * tile + side) * 64
            out_ref[base : base + 32, :] = block
            out_ref[base + 32 : base + 64, :] = gram


def packed(zs, own, got):
    return pl.pallas_call(
        lambda *refs: packing(zs, *refs),
        out_shape=jax.ShapeDtypeStruct((zs * 64, LANES), jnp.float32),
        compiler_params=pltpu.CompilerParams(vmem_limit_bytes=8 * MIB),
        name="packing",
    )(own, got)


def iterating(zs, members, got_ref, start_ref, out_ref):
    total = got_ref[0:64, :]
    for part in range(1, zs):
        total = total + got_ref[part * 64 : part * 64 + 64, :]
    target = unstack(total[:32])
    gram = unstack(total[32:])[:, :HALF]
    lip = jnp.max(jnp.sum(gram, axis=1, keepdims=True))
    factor = start_ref[...]
    ahead = factor
    momentum = 1.0
    for step in range(ITERS):
        slope = jnp.dot(
            gram, ahead, precision=lax.Precision.HIGHEST, preferred_element_type=jnp.float32
        ) - target
        fresh = jnp.maximum(ahead - slope / lip, 0.0)
        following = (1.0 + math.sqrt(1.0 + 4.0 * momentum * momentum)) / 2.0
        ahead = fresh + (momentum - 1.0) / following * (fresh - factor)
        factor = fresh
        momentum = following
    block = stack_sides(factor)
    for part in range(members):
        out_ref[part * 32 : part * 32 + 32, :] = block


def iterated(zs, members, got, start):
    return pl.pallas_call(
        lambda *refs: iterating(zs, members, *refs),
        out_shape=jax.ShapeDtypeStruct((members * 32, LANES), jnp.float32),
        compiler_params=pltpu.CompilerParams(vmem_limit_bytes=8 * MIB),
        name="iterating",
    )(got, start)


def fold_masks(shape):
    row = lax.broadcasted_iota(jnp.int32, shape, 0)
    lane = lax.broadcasted_iota(jnp.int32, shape, 1)
    row = row + jnp.where(lane < HALF, 0, 16)
    return lane % HALF < 32, row > lane % 32


def contracting(zs, got_ref, data_ref, factor_ref, out_ref, lines):
    width = zs * HALF
    for side in range(2):
        for pair in range(zs // 2):
            first, second = (2 * (2 * pair) + side) * 32, (2 * (2 * pair + 1) + side) * 32
            a = got_ref[first : first + 32, :]
            b = got_ref[second : second + 32, :]
            left = low_lanes(a)
            x = jnp.concatenate([jnp.where(left, a, turned(b)), jnp.where(left, turned(a), b)], axis=0)
            at = slice(side * width + pair * LANES, side * width + (pair + 1) * LANES)
            factor_ref[:, at] = x
            low = x.astype(jnp.bfloat16)
            lines[0:64, at] = low
            lines[64:128, at] = low
    factor = factor_ref[...]
    squares = jnp.sum(factor * factor, axis=1, keepdims=True)
    both = (((1,), (1,)), ((), ()))
    outer = lax.dot_general(lines[0:64, :], lines[...], both, preferred_element_type=jnp.float32)
    ones = jnp.ones((8, lines.shape[1]), jnp.bfloat16)
    sums = lax.dot_general(ones, lines[...], both, preferred_element_type=jnp.float32)[0:1, :]
    power = jnp.ceil(jnp.log(jnp.maximum(sums, 1e-30)) * LOG2E)
    power = jnp.clip(power, -60.0, 60.0)
    most = jnp.max(power, axis=1, keepdims=True)
    shrink = jnp.exp2(-power)
    row = lax.broadcasted_iota(jnp.int32, outer.shape, 0)
    lane = lax.broadcasted_iota(jnp.int32, outer.shape, 1)
    across = jnp.sum(jnp.where(row == lane % HALF, squares, 0.0), axis=0, keepdims=True)
    across = across * shrink * shrink * 32768.0
    wide = across * 8193.0
    high = wide - (wide - across)
    line = lax.broadcasted_iota(jnp.int32, (8, LANES), 0)
    extra = jnp.where(
        line == 0,
        jnp.where(low_lanes(high), high, across - high),
        jnp.where(line == 1, power, jnp.where(line == 2, power + most, 0.0)),
    )
    outer = outer * (shrink * jnp.exp2(-most) * 32768.0)
    top, low = outer[:32], outer[32:]
    lane = lax.broadcasted_iota(jnp.int32, top.shape, 1)
    row = lax.broadcasted_iota(jnp.int32, top.shape, 0)
    folded = jnp.where((lane % HALF < 32) & (row > lane % 32), pltpu.roll(low, 96, 1), top)
    folded = jnp.where(low_lanes(folded[:16]), folded[:16], folded[16:])
    shrink = shrink * 1024.0

    parts = data_ref.shape[0] // 64
    each = parts // BLOCKS
    for block in range(BLOCKS):
        at = slice(block * each * 64, (block + 1) * each * 64)
        terms = lax.dot_general(data_ref[at, :], lines[...], both, preferred_element_type=jnp.float32) * shrink
        for part in range(each):
            base = (block * each + part) * CHUNK
            out_ref[base : base + 32, :] = stack_copies(terms[part * 64 : part * 64 + 64])
            out_ref[base + 32 : base + 48, :] = folded
            out_ref[base + 48 : base + 56, :] = extra


def contracted(zs, got, data):
    rows, columns = data.shape
    return pl.pallas_call(
        lambda *refs: contracting(zs, *refs),
        out_shape=[
            jax.ShapeDtypeStruct((64, columns), jnp.float32),
            jax.ShapeDtypeStruct((rows // 64 * CHUNK, LANES), jnp.float32),
        ],
        in_specs=[pl.BlockSpec(memory_space=pltpu.VMEM)] * 2,
        out_specs=[pl.BlockSpec(memory_space=pltpu.VMEM)] * 2,
        scratch_shapes=[pltpu.VMEM((LANES, columns), jnp.bfloat16)],
        compiler_params=pltpu.CompilerParams(vmem_limit_bytes=16 * MIB),
        name="contracting",
    )(got, data)


def finishing(count, columns, got_ref, factor_ref, scaled_ref, gram_ref, terms_ref):
    folded_in, lower = fold_masks((16, LANES))
    swapped = folded_in & lower
    terms = jnp.zeros((32, LANES), jnp.float32)
    folded = jnp.zeros((16, LANES), jnp.float32)
    squares = jnp.zeros((1, LANES), jnp.float32)
    for part in range(count):
        base = part * CHUNK
        extra = got_ref[base + 48 : base + 56, :]
        grown = jnp.exp2(extra[1:3, :])
        grow, pair = grown[0:1], grown[1:2]
        terms = terms + got_ref[base : base + 32, :] * grow
        folded = folded + got_ref[base + 32 : base + 48, :] * jnp.where(swapped, pltpu.roll(pair, 96, 1), pair)
        squares = squares + (extra[0:1, :] + turned(extra[0:1, :])) * (grow * grow)
    squares = squares[:, :HALF] * (1.0 / 32768.0)
    upper = jnp.concatenate([folded, turned(folded)], axis=0) * (1.0 / 32768.0)
    upper = jnp.concatenate([upper, pltpu.roll(upper, 32, 1)], axis=0)
    mirror = jnp.transpose(upper)[:HALF, :]
    upper = upper[:, :HALF]
    row = lax.broadcasted_iota(jnp.int32, upper.shape, 0)
    lane = lax.broadcasted_iota(jnp.int32, upper.shape, 1)
    held = ((row < 32) & (row < lane)) | ((lane >= 32) & (row > lane))
    outer = jnp.where(row == lane, squares, jnp.where(held, upper, mirror))

    def scale_of(squares):
        mean = squares / columns + 1e-06
        first = lax.rsqrt(mean)
        return first * (1.5 - 0.5 * mean * first * first)

    across = scale_of(squares)
    down = scale_of(jnp.sum(jnp.where(row == lane, squares, 0.0), axis=1, keepdims=True))
    scaled_ref[...] = (factor_ref[...] * down).astype(jnp.bfloat16)
    gram_ref[...] = outer * down * across / columns
    terms = jnp.transpose(unstack(terms))[:HALF, :]
    terms_ref[...] = terms * down * (1.0 / 1024.0) / columns


def finished(count, columns, got, factor):
    return pl.pallas_call(
        lambda *refs: finishing(count, columns, *refs),
        out_shape=[
            jax.ShapeDtypeStruct(factor.shape, jnp.bfloat16),
            jax.ShapeDtypeStruct((64, 64), jnp.float32),
            jax.ShapeDtypeStruct((64, 64), jnp.float32),
        ],
        compiler_params=pltpu.CompilerParams(vmem_limit_bytes=8 * MIB),
        name="finishing",
    )(got, factor)


def shards(data, w_rows, h_init):
    members = lax.axis_size("row")
    zs = members // 2
    count = lax.axis_size("col")
    columns = data.shape[1] * count
    swap = [(2 * z + c, 2 * z + 1 - c) for z in range(zs) for c in range(2)]
    levels = [[2 * z + c for z in range(zs)] for c in range(2)]

    own, send, start = multiplied(zs, w_rows, data, h_init)
    got = lax.ppermute(send, "row", swap)
    parts = packed(zs, own, got)
    parts = lax.all_to_all(parts, "row", 0, 0, tiled=True, axis_index_groups=levels)
    copies = iterated(zs, members, parts, start)
    blocks = lax.all_to_all(copies, "row", 0, 0, tiled=True)
    factor, terms = contracted(zs, blocks, data)
    sums = lax.all_to_all(terms.astype(jnp.float16), "col", 0, 0, tiled=True)
    return tuple(finished(count, columns, sums.astype(jnp.float32), factor))


def solution(mesh):
    in_specs = (P("row", "col"), P(None, "row"), P(None, "col"))
    out_specs = (P(None, "col"), P(), P(None, ("row", "col")))
    return jax.shard_map(shards, mesh=mesh, in_specs=in_specs, out_specs=out_specs, check_vma=False)
```

```python
import math

import jax
import jax.numpy as jnp
from jax import lax
from jax.experimental import pallas as pl
from jax.experimental.pallas import tpu as pltpu
from jax.sharding import PartitionSpec as P

ITERS = 4
LOG2E = 1.4426950408889634
LANES = 128
HALF = 64
BLOCKS = 4
GRANT = 55947264
CHUNK = 56
MIB = 1 << 20


def low_lanes(x):
    return lax.broadcasted_iota(jnp.int32, x.shape, 1) < HALF


def turned(x):
    return pltpu.roll(x, HALF, 1)


def stack_sides(x):
    return jnp.where(low_lanes(x[:32]), x[:32], turned(x[32:]))


def stack_copies(x):
    return jnp.where(low_lanes(x[:32]), x[:32], x[32:])


def unstack(x):
    return jnp.concatenate([x, turned(x)], axis=0)


def sending(w_hbm, data_hbm, h_hbm, send_ref, start_ref, w, data_ref, h, acc, sems):
    rows, width = data_ref.shape
    depth = rows // BLOCKS
    me = lax.axis_index("row")
    core, level = lax.rem(me, 2), lax.div(me, 2)
    theirs = pl.multiple_of((1 - core) * width, LANES)
    tile = core * (width // LANES) + lax.div(level, 2)
    copies = [pltpu.make_async_copy(w_hbm, w, sems.at[BLOCKS])]
    for block in range(BLOCKS):
        at = pl.ds(block * depth, depth)
        copies.append(
            pltpu.make_async_copy(data_hbm.at[at, pl.ds(theirs, width)], data_ref.at[at, :], sems.at[block])
        )
    copies.append(
        pltpu.make_async_copy(
            h_hbm.at[:, pl.ds(pl.multiple_of(tile * LANES, LANES), LANES)], h, sems.at[BLOCKS + 1]
        )
    )
    for copy in copies:
        copy.start()
    copies[0].wait()
    send_ref[:, width:] = lax.dot_general(
        w[...], jnp.concatenate([w[...], w[...]], axis=0), (((1,), (1,)), ((), ())), preferred_element_type=jnp.float32
    )
    for block in range(BLOCKS):
        copies[1 + block].wait()
        at = slice(block * depth, (block + 1) * depth)
        part = jnp.dot(w[:, at], data_ref[at, :], preferred_element_type=jnp.float32)
        if block == 0:
            acc[...] = part
        elif block < BLOCKS - 1:
            acc[...] += part
        else:
            send_ref[:, :width] = acc[...] + part
    copies[BLOCKS + 1].wait()
    begin = h[...]
    start_ref[...] = jnp.where(lax.rem(level, 2) == 0, begin, turned(begin))


def sent(w_rows, data, h_init):
    rows, columns = data.shape
    rank, width = w_rows.shape[0], columns // 2
    return pl.pallas_call(
        sending,
        in_specs=[pl.BlockSpec(memory_space=pl.ANY)] * 3,
        out_specs=[pl.BlockSpec(memory_space=pltpu.VMEM)] * 3,
        out_shape=[
            jax.ShapeDtypeStruct((rank, width + LANES), jnp.float32),
            jax.ShapeDtypeStruct((rank, LANES), jnp.float32),
            jax.ShapeDtypeStruct(w_rows.shape, w_rows.dtype),
        ],
        scratch_shapes=[
            pltpu.VMEM((rows, width), data.dtype),
            pltpu.VMEM((rank, LANES), jnp.float32),
            pltpu.VMEM((rank, width), jnp.float32),
            pltpu.SemaphoreType.DMA((BLOCKS + 2,)),
        ],
        compiler_params=pltpu.CompilerParams(vmem_limit_bytes=GRANT),
        name="sending",
    )(w_rows, data, h_init)


def keeping(w_ref, data_ref, own_ref):
    width = own_ref.shape[1]
    mine = pl.multiple_of(lax.rem(lax.axis_index("row"), 2) * width, LANES)
    own_ref[...] = jnp.dot(w_ref[...], data_ref[:, pl.ds(mine, width)], preferred_element_type=jnp.float32)


def kept(w_rows, data):
    return pl.pallas_call(
        keeping,
        in_specs=[pl.BlockSpec(memory_space=pltpu.VMEM)] * 2,
        out_specs=pl.BlockSpec(memory_space=pltpu.VMEM),
        out_shape=jax.ShapeDtypeStruct((w_rows.shape[0], data.shape[1] // 2), jnp.float32),
        compiler_params=pltpu.CompilerParams(vmem_limit_bytes=8 * MIB),
        name="keeping",
    )(w_rows, data)


def packing(zs, own_ref, send_ref, got_ref, out_ref):
    width = own_ref.shape[1]
    gram = stack_copies(send_ref[:, width:] + got_ref[:, width:])
    for tile in range(width // LANES):
        at = slice(tile * LANES, (tile + 1) * LANES)
        x = own_ref[:, at] + got_ref[:, at]
        top, low = x[:32], x[32:]
        left = low_lanes(top)
        for side, block in enumerate((jnp.where(left, top, turned(low)), jnp.where(left, turned(top), low))):
            base = (2 * tile + side) * 64
            out_ref[base : base + 32, :] = block
            out_ref[base + 32 : base + 64, :] = gram


def packed(zs, own, send, got):
    return pl.pallas_call(
        lambda *refs: packing(zs, *refs),
        out_shape=jax.ShapeDtypeStruct((zs * 64, LANES), jnp.float32),
        compiler_params=pltpu.CompilerParams(vmem_limit_bytes=8 * MIB),
        name="packing",
    )(own, send, got)


def iterating(zs, members, got_ref, start_ref, out_ref):
    total = got_ref[0:64, :]
    for part in range(1, zs):
        total = total + got_ref[part * 64 : part * 64 + 64, :]
    target = unstack(total[:32])
    gram = unstack(total[32:])[:, :HALF]
    lip = jnp.max(jnp.sum(gram, axis=1, keepdims=True))
    factor = start_ref[...]
    ahead = factor
    momentum = 1.0
    for step in range(ITERS):
        slope = jnp.dot(
            gram, ahead, precision=lax.Precision.HIGHEST, preferred_element_type=jnp.float32
        ) - target
        fresh = jnp.maximum(ahead - slope / lip, 0.0)
        following = (1.0 + math.sqrt(1.0 + 4.0 * momentum * momentum)) / 2.0
        ahead = fresh + (momentum - 1.0) / following * (fresh - factor)
        factor = fresh
        momentum = following
    block = stack_sides(factor)
    for part in range(members):
        out_ref[part * 32 : part * 32 + 32, :] = block


def iterated(zs, members, got, start):
    return pl.pallas_call(
        lambda *refs: iterating(zs, members, *refs),
        out_shape=jax.ShapeDtypeStruct((members * 32, LANES), jnp.float32),
        compiler_params=pltpu.CompilerParams(vmem_limit_bytes=8 * MIB),
        name="iterating",
    )(got, start)


def fold_masks(shape):
    row = lax.broadcasted_iota(jnp.int32, shape, 0)
    lane = lax.broadcasted_iota(jnp.int32, shape, 1)
    row = row + jnp.where(lane < HALF, 0, 16)
    return lane % HALF < 32, row > lane % 32


BOTH = (((1,), (1,)), ((), ()))


def unpacking(zs, got_ref):
    for pair in range(zs // 2):
        a = got_ref[pair * 64 : pair * 64 + 32, :]
        b = got_ref[pair * 64 + 32 : pair * 64 + 64, :]
        left = low_lanes(a)
        yield jnp.concatenate([jnp.where(left, a, turned(b)), jnp.where(left, turned(a), b)], axis=0)


def starting(zs, got_ref, data_ref, factor_ref, terms_ref, lines):
    width = zs * HALF
    mine = pl.multiple_of(lax.rem(lax.axis_index("row"), 2) * width, LANES)
    for pair, x in enumerate(unpacking(zs, got_ref)):
        at = slice(pair * LANES, (pair + 1) * LANES)
        factor_ref[:, at] = x
        low = x.astype(jnp.bfloat16)
        lines[0:64, at] = low
        lines[64:128, at] = low
    step = data_ref.shape[0] // BLOCKS
    for block in range(BLOCKS):
        at = slice(block * step, (block + 1) * step)
        terms_ref[at, :] = lax.dot_general(
            data_ref[at, pl.ds(mine, width)], lines[...], BOTH, preferred_element_type=jnp.float32
        )


def started(zs, got, data):
    width = zs * HALF
    return pl.pallas_call(
        lambda *refs: starting(zs, *refs),
        out_shape=[
            jax.ShapeDtypeStruct((64, width), jnp.float32),
            jax.ShapeDtypeStruct((data.shape[0], LANES), jnp.float32),
        ],
        in_specs=[pl.BlockSpec(memory_space=pltpu.VMEM)] * 2,
        out_specs=[pl.BlockSpec(memory_space=pltpu.VMEM)] * 2,
        scratch_shapes=[pltpu.VMEM((LANES, width), jnp.bfloat16)],
        compiler_params=pltpu.CompilerParams(vmem_limit_bytes=8 * MIB),
        name="starting",
    )(got, data)


def contracting(zs, got_ref, half_ref, begun_ref, data_ref, factor_ref, out_ref, lines):
    width = zs * HALF
    core = lax.rem(lax.axis_index("row"), 2)
    mine = pl.multiple_of(core * width, LANES)
    theirs = pl.multiple_of((1 - core) * width, LANES)
    half = half_ref[...]
    factor_ref[:, pl.ds(mine, width)] = half
    for pair, x in enumerate(unpacking(zs, got_ref)):
        at = slice(pair * LANES, (pair + 1) * LANES)
        factor_ref[:, pl.ds(pl.multiple_of(theirs + pair * LANES, LANES), LANES)] = x
        low = x.astype(jnp.bfloat16)
        lines[0:64, at] = low
        lines[64:128, at] = low
    low = half.astype(jnp.bfloat16)
    lines[0:64, width:] = low
    lines[64:128, width:] = low
    factor = factor_ref[...]
    squares = jnp.sum(factor * factor, axis=1, keepdims=True)
    outer = lax.dot_general(lines[0:64, :], lines[...], BOTH, preferred_element_type=jnp.float32)
    ones = jnp.ones((8, lines.shape[1]), jnp.bfloat16)
    sums = lax.dot_general(ones, lines[...], BOTH, preferred_element_type=jnp.float32)[0:1, :]
    power = jnp.ceil(jnp.log(jnp.maximum(sums, 1e-30)) * LOG2E)
    power = jnp.clip(power, -60.0, 60.0)
    most = jnp.max(power, axis=1, keepdims=True)
    shrink = jnp.exp2(-power)
    row = lax.broadcasted_iota(jnp.int32, outer.shape, 0)
    lane = lax.broadcasted_iota(jnp.int32, outer.shape, 1)
    across = jnp.sum(jnp.where(row == lane % HALF, squares, 0.0), axis=0, keepdims=True)
    across = across * shrink * shrink * 32768.0
    wide = across * 8193.0
    high = wide - (wide - across)
    line = lax.broadcasted_iota(jnp.int32, (8, LANES), 0)
    extra = jnp.where(
        line == 0,
        jnp.where(low_lanes(high), high, across - high),
        jnp.where(line == 1, power, jnp.where(line == 2, power + most, 0.0)),
    )
    outer = outer * (shrink * jnp.exp2(-most) * 32768.0)
    top, low = outer[:32], outer[32:]
    lane = lax.broadcasted_iota(jnp.int32, top.shape, 1)
    row = lax.broadcasted_iota(jnp.int32, top.shape, 0)
    folded = jnp.where((lane % HALF < 32) & (row > lane % 32), pltpu.roll(low, 96, 1), top)
    folded = jnp.where(low_lanes(folded[:16]), folded[:16], folded[16:])
    shrink = shrink * 1024.0

    parts = data_ref.shape[0] // 64
    each = parts // BLOCKS
    for block in range(BLOCKS):
        at = slice(block * each * 64, (block + 1) * each * 64)
        terms = lax.dot_general(
            data_ref[at, pl.ds(theirs, width)], lines[:, :width], BOTH, preferred_element_type=jnp.float32
        )
        terms = (terms + begun_ref[at, :]) * shrink
        for part in range(each):
            base = (block * each + part) * CHUNK
            out_ref[base : base + 32, :] = stack_copies(terms[part * 64 : part * 64 + 64])
            out_ref[base + 32 : base + 48, :] = folded
            out_ref[base + 48 : base + 56, :] = extra


def contracted(zs, got, half, begun, data):
    rows, columns = data.shape
    return pl.pallas_call(
        lambda *refs: contracting(zs, *refs),
        out_shape=[
            jax.ShapeDtypeStruct((64, columns), jnp.float32),
            jax.ShapeDtypeStruct((rows // 64 * CHUNK, LANES), jnp.float32),
        ],
        in_specs=[pl.BlockSpec(memory_space=pltpu.VMEM)] * 4,
        out_specs=[pl.BlockSpec(memory_space=pltpu.VMEM)] * 2,
        scratch_shapes=[pltpu.VMEM((LANES, columns), jnp.bfloat16)],
        compiler_params=pltpu.CompilerParams(vmem_limit_bytes=16 * MIB),
        name="contracting",
    )(got, half, begun, data)


def finishing(count, columns, got_ref, factor_ref, scaled_ref, gram_ref, terms_ref):
    folded_in, lower = fold_masks((16, LANES))
    swapped = folded_in & lower
    terms = jnp.zeros((32, LANES), jnp.float32)
    folded = jnp.zeros((16, LANES), jnp.float32)
    squares = jnp.zeros((1, LANES), jnp.float32)
    for part in range(count):
        base = part * CHUNK
        extra = got_ref[base + 48 : base + 56, :]
        grown = jnp.exp2(extra[1:3, :])
        grow, pair = grown[0:1], grown[1:2]
        terms = terms + got_ref[base : base + 32, :] * grow
        folded = folded + got_ref[base + 32 : base + 48, :] * jnp.where(swapped, pltpu.roll(pair, 96, 1), pair)
        squares = squares + (extra[0:1, :] + turned(extra[0:1, :])) * (grow * grow)
    squares = squares[:, :HALF] * (1.0 / 32768.0)
    upper = jnp.concatenate([folded, turned(folded)], axis=0) * (1.0 / 32768.0)
    upper = jnp.concatenate([upper, pltpu.roll(upper, 32, 1)], axis=0)
    mirror = jnp.transpose(upper)[:HALF, :]
    upper = upper[:, :HALF]
    row = lax.broadcasted_iota(jnp.int32, upper.shape, 0)
    lane = lax.broadcasted_iota(jnp.int32, upper.shape, 1)
    held = ((row < 32) & (row < lane)) | ((lane >= 32) & (row > lane))
    outer = jnp.where(row == lane, squares, jnp.where(held, upper, mirror))

    def scale_of(squares):
        mean = squares / columns + 1e-06
        first = lax.rsqrt(mean)
        return first * (1.5 - 0.5 * mean * first * first)

    across = scale_of(squares)
    down = scale_of(jnp.sum(jnp.where(row == lane, squares, 0.0), axis=1, keepdims=True))
    scaled_ref[...] = (factor_ref[...] * down).astype(jnp.bfloat16)
    gram_ref[...] = outer * down * across / columns
    terms = jnp.transpose(unstack(terms))[:HALF, :]
    terms_ref[...] = terms * down * (1.0 / 1024.0) / columns


def finished(count, columns, got, factor):
    return pl.pallas_call(
        lambda *refs: finishing(count, columns, *refs),
        out_shape=[
            jax.ShapeDtypeStruct(factor.shape, jnp.bfloat16),
            jax.ShapeDtypeStruct((64, 64), jnp.float32),
            jax.ShapeDtypeStruct((64, 64), jnp.float32),
        ],
        compiler_params=pltpu.CompilerParams(vmem_limit_bytes=8 * MIB),
        name="finishing",
    )(got, factor)


def shards(data, w_rows, h_init):
    members = lax.axis_size("row")
    zs = members // 2
    count = lax.axis_size("col")
    columns = data.shape[1] * count
    swap = [(2 * z + c, 2 * z + 1 - c) for z in range(zs) for c in range(2)]
    levels = [[2 * z + c for z in range(zs)] for c in range(2)]

    send, start, w_rows = sent(w_rows, data, h_init)
    got = lax.ppermute(send, "row", swap)
    own = kept(w_rows, data)
    parts = packed(zs, own, send, got)
    parts = lax.all_to_all(parts, "row", 0, 0, tiled=True, axis_index_groups=levels)
    copies = iterated(zs, zs, parts, start)
    blocks = lax.all_to_all(copies, "row", 0, 0, tiled=True, axis_index_groups=levels)
    others = lax.ppermute(blocks, "row", swap)
    half, begun = started(zs, blocks, data)
    factor, terms = contracted(zs, others, half, begun, data)
    sums = lax.all_to_all(terms.astype(jnp.float16), "col", 0, 0, tiled=True)
    return tuple(finished(count, columns, sums.astype(jnp.float32), factor))


def solution(mesh):
    in_specs = (P("row", "col"), P(None, "row"), P(None, "col"))
    out_specs = (P(None, "col"), P(), P(None, ("row", "col")))
    return jax.shard_map(shards, mesh=mesh, in_specs=in_specs, out_specs=out_specs, check_vma=False)
```

```python
import math

import jax
import jax.numpy as jnp
from jax import lax
from jax.experimental import pallas as pl
from jax.experimental.pallas import tpu as pltpu
from jax.sharding import PartitionSpec as P

ITERS = 4
LOG2E = 1.4426950408889634
LANES = 128
HALF = 64
BLOCKS = 4
CHUNK = 56
MIB = 1 << 20


def low_lanes(x):
    return lax.broadcasted_iota(jnp.int32, x.shape, 1) < HALF


def turned(x):
    return pltpu.roll(x, HALF, 1)


def stack_sides(x):
    return jnp.where(low_lanes(x[:32]), x[:32], turned(x[32:]))


def stack_copies(x):
    return jnp.where(low_lanes(x[:32]), x[:32], x[32:])


def unstack(x):
    return jnp.concatenate([x, turned(x)], axis=0)


def multiplying(zs, w_hbm, data_hbm, h_hbm, own_ref, send_ref, start_ref, data_ref, w, h, acc, sems):
    rows, columns = data_ref.shape
    width = columns // 2
    depth = rows // BLOCKS
    me = lax.axis_index("row")
    core, level = lax.rem(me, 2), lax.div(me, 2)
    tile = core * (width // LANES) + lax.div(level, 2)
    copies = [
        pltpu.make_async_copy(w_hbm, w, sems.at[BLOCKS]),
        pltpu.make_async_copy(
            h_hbm.at[:, pl.ds(pl.multiple_of(tile * LANES, LANES), LANES)], h, sems.at[BLOCKS + 1]
        ),
    ]
    for block in range(BLOCKS):
        at = pl.ds(block * depth, depth)
        copies.append(pltpu.make_async_copy(data_hbm.at[at, :], data_ref.at[at, :], sems.at[block]))
    for copy in (copies[0], *copies[2:], copies[1]):
        copy.start()
    copies[0].wait()
    gram = lax.dot_general(
        w[...], jnp.concatenate([w[...], w[...]], axis=0), (((1,), (1,)), ((), ())), preferred_element_type=jnp.float32
    )
    own_ref[:, width:] = gram
    send_ref[:, width:] = gram
    for block in range(BLOCKS):
        copies[2 + block].wait()
        at = slice(block * depth, (block + 1) * depth)
        part = jnp.dot(w[:, at], data_ref[at, :], preferred_element_type=jnp.float32)
        if block == 0:
            acc[...] = part
        else:
            acc[...] += part
    first = core == 0
    left = acc[:, :width]
    right = acc[:, width:]
    own_ref[:, :width] = jnp.where(first, left, right)
    send_ref[:, :width] = jnp.where(first, right, left)
    copies[1].wait()
    begin = h[...]
    start_ref[...] = jnp.where(lax.rem(level, 2) == 0, begin, turned(begin))


def multiplied(zs, w_rows, data, h_init):
    rows, columns = data.shape
    rank = w_rows.shape[0]
    half = jax.ShapeDtypeStruct((rank, columns // 2 + LANES), jnp.float32)
    start = jax.ShapeDtypeStruct((rank, LANES), jnp.float32)
    return pl.pallas_call(
        lambda *refs: multiplying(zs, *refs),
        in_specs=[pl.BlockSpec(memory_space=pl.ANY)] * 3,
        out_specs=[pl.BlockSpec(memory_space=pltpu.VMEM)] * 3,
        out_shape=[half, half, start],
        scratch_shapes=[
            pltpu.VMEM(data.shape, data.dtype),
            pltpu.VMEM(w_rows.shape, w_rows.dtype),
            pltpu.VMEM((rank, LANES), jnp.float32),
            pltpu.VMEM((rank, columns), jnp.float32),
            pltpu.SemaphoreType.DMA((BLOCKS + 2,)),
        ],
        compiler_params=pltpu.CompilerParams(vmem_limit_bytes=56045568),
        name="multiplying",
    )(w_rows, data, h_init)


def packing(zs, own_ref, got_ref, out_ref):
    width = own_ref.shape[1] - LANES
    rank = own_ref.shape[0]
    theirs = pl.ds(pl.multiple_of((1 - lax.rem(lax.axis_index("row"), 2)) * rank, 8), rank)
    gram = stack_copies(own_ref[:, width:] + got_ref[theirs, width:])
    for tile in range(width // LANES):
        at = slice(tile * LANES, (tile + 1) * LANES)
        x = own_ref[:, at] + got_ref[theirs, at]
        top, low = x[:32], x[32:]
        left = low_lanes(top)
        for side, block in enumerate((jnp.where(left, top, turned(low)), jnp.where(left, turned(top), low))):
            base = (2 * tile + side) * 64
            out_ref[base : base + 32, :] = block
            out_ref[base + 32 : base + 64, :] = gram


def packed(zs, own, got):
    return pl.pallas_call(
        lambda *refs: packing(zs, *refs),
        out_shape=jax.ShapeDtypeStruct((zs * 64, LANES), jnp.float32),
        compiler_params=pltpu.CompilerParams(vmem_limit_bytes=8 * MIB),
        name="packing",
    )(own, got)


def iterating(zs, got_ref, start_ref, out_ref):
    total = got_ref[0:64, :]
    for part in range(1, zs):
        total = total + got_ref[part * 64 : part * 64 + 64, :]
    target = unstack(total[:32])
    gram = unstack(total[32:])[:, :HALF]
    lip = jnp.max(jnp.sum(gram, axis=1, keepdims=True))
    factor = start_ref[...]
    ahead = factor
    momentum = 1.0
    for step in range(ITERS):
        slope = jnp.dot(
            gram, ahead, precision=lax.Precision.HIGHEST, preferred_element_type=jnp.float32
        ) - target
        fresh = jnp.maximum(ahead - slope / lip, 0.0)
        following = (1.0 + math.sqrt(1.0 + 4.0 * momentum * momentum)) / 2.0
        ahead = fresh + (momentum - 1.0) / following * (fresh - factor)
        factor = fresh
        momentum = following
    block = stack_sides(factor)
    for part in range(zs):
        out_ref[part * 32 : part * 32 + 32, :] = block


def iterated(zs, got, start):
    return pl.pallas_call(
        lambda *refs: iterating(zs, *refs),
        out_shape=jax.ShapeDtypeStruct((zs * 32, LANES), jnp.float32),
        compiler_params=pltpu.CompilerParams(vmem_limit_bytes=8 * MIB),
        name="iterating",
    )(got, start)


def fold_masks(shape):
    row = lax.broadcasted_iota(jnp.int32, shape, 0)
    lane = lax.broadcasted_iota(jnp.int32, shape, 1)
    row = row + jnp.where(lane < HALF, 0, 16)
    return lane % HALF < 32, row > lane % 32


def contracting(zs, got_ref, data_ref, factor_ref, out_ref, lines):
    width = zs * HALF
    for side in range(2):
        for pair in range(zs // 2):
            first = (side * zs + 2 * pair) * 32
            second = first + 32
            a = got_ref[first : first + 32, :]
            b = got_ref[second : second + 32, :]
            left = low_lanes(a)
            x = jnp.concatenate([jnp.where(left, a, turned(b)), jnp.where(left, turned(a), b)], axis=0)
            at = slice(side * width + pair * LANES, side * width + (pair + 1) * LANES)
            factor_ref[:, at] = x
            low = x.astype(jnp.bfloat16)
            lines[0:64, at] = low
            lines[64:128, at] = low
    factor = factor_ref[...]
    squares = jnp.sum(factor * factor, axis=1, keepdims=True)
    both = (((1,), (1,)), ((), ()))
    outer = lax.dot_general(lines[0:64, :], lines[...], both, preferred_element_type=jnp.float32)
    ones = jnp.ones((8, lines.shape[1]), jnp.bfloat16)
    sums = lax.dot_general(ones, lines[...], both, preferred_element_type=jnp.float32)[0:1, :]
    power = jnp.ceil(jnp.log(jnp.maximum(sums, 1e-30)) * LOG2E)
    power = jnp.clip(power, -60.0, 60.0)
    most = jnp.max(power, axis=1, keepdims=True)
    shrink = jnp.exp2(-power)
    row = lax.broadcasted_iota(jnp.int32, outer.shape, 0)
    lane = lax.broadcasted_iota(jnp.int32, outer.shape, 1)
    across = jnp.sum(jnp.where(row == lane % HALF, squares, 0.0), axis=0, keepdims=True)
    across = across * shrink * shrink * 32768.0
    wide = across * 8193.0
    high = wide - (wide - across)
    line = lax.broadcasted_iota(jnp.int32, (8, LANES), 0)
    extra = jnp.where(
        line == 0,
        jnp.where(low_lanes(high), high, across - high),
        jnp.where(line == 1, power, jnp.where(line == 2, power + most, 0.0)),
    )
    outer = outer * (shrink * jnp.exp2(-most) * 32768.0)
    top, low = outer[:32], outer[32:]
    lane = lax.broadcasted_iota(jnp.int32, top.shape, 1)
    row = lax.broadcasted_iota(jnp.int32, top.shape, 0)
    folded = jnp.where((lane % HALF < 32) & (row > lane % 32), pltpu.roll(low, 96, 1), top)
    folded = jnp.where(low_lanes(folded[:16]), folded[:16], folded[16:])
    shrink = shrink * 1024.0

    parts = data_ref.shape[0] // 64
    each = parts // BLOCKS
    for block in range(BLOCKS):
        at = slice(block * each * 64, (block + 1) * each * 64)
        terms = lax.dot_general(data_ref[at, :], lines[...], both, preferred_element_type=jnp.float32) * shrink
        for part in range(each):
            base = (block * each + part) * CHUNK
            out_ref[base : base + 32, :] = stack_copies(terms[part * 64 : part * 64 + 64])
            out_ref[base + 32 : base + 48, :] = folded
            out_ref[base + 48 : base + 56, :] = extra


def contracted(zs, got, data):
    rows, columns = data.shape
    return pl.pallas_call(
        lambda *refs: contracting(zs, *refs),
        out_shape=[
            jax.ShapeDtypeStruct((64, columns), jnp.float32),
            jax.ShapeDtypeStruct((rows // 64 * CHUNK, LANES), jnp.float32),
        ],
        in_specs=[pl.BlockSpec(memory_space=pltpu.VMEM)] * 2,
        out_specs=[pl.BlockSpec(memory_space=pltpu.VMEM)] * 2,
        scratch_shapes=[pltpu.VMEM((LANES, columns), jnp.bfloat16)],
        compiler_params=pltpu.CompilerParams(vmem_limit_bytes=16 * MIB),
        name="contracting",
    )(got, data)


def finishing(count, columns, got_ref, factor_ref, scaled_ref, gram_ref, terms_ref):
    folded_in, lower = fold_masks((16, LANES))
    swapped = folded_in & lower
    terms = jnp.zeros((32, LANES), jnp.float32)
    folded = jnp.zeros((16, LANES), jnp.float32)
    squares = jnp.zeros((1, LANES), jnp.float32)
    for part in range(count):
        base = part * CHUNK
        extra = got_ref[base + 48 : base + 56, :]
        grown = jnp.exp2(extra[1:3, :])
        grow, pair = grown[0:1], grown[1:2]
        terms = terms + got_ref[base : base + 32, :] * grow
        folded = folded + got_ref[base + 32 : base + 48, :] * jnp.where(swapped, pltpu.roll(pair, 96, 1), pair)
        squares = squares + (extra[0:1, :] + turned(extra[0:1, :])) * (grow * grow)
    squares = squares[:, :HALF] * (1.0 / 32768.0)
    upper = jnp.concatenate([folded, turned(folded)], axis=0) * (1.0 / 32768.0)
    upper = jnp.concatenate([upper, pltpu.roll(upper, 32, 1)], axis=0)
    mirror = jnp.transpose(upper)[:HALF, :]
    upper = upper[:, :HALF]
    row = lax.broadcasted_iota(jnp.int32, upper.shape, 0)
    lane = lax.broadcasted_iota(jnp.int32, upper.shape, 1)
    held = ((row < 32) & (row < lane)) | ((lane >= 32) & (row > lane))
    outer = jnp.where(row == lane, squares, jnp.where(held, upper, mirror))

    def scale_of(squares):
        mean = squares / columns + 1e-06
        first = lax.rsqrt(mean)
        return first * (1.5 - 0.5 * mean * first * first)

    across = scale_of(squares)
    down = scale_of(jnp.sum(jnp.where(row == lane, squares, 0.0), axis=1, keepdims=True))
    scaled_ref[...] = (factor_ref[...] * down).astype(jnp.bfloat16)
    gram_ref[...] = outer * down * across / columns
    terms = jnp.transpose(unstack(terms))[:HALF, :]
    terms_ref[...] = terms * down * (1.0 / 1024.0) / columns


def finished(count, columns, got, factor):
    return pl.pallas_call(
        lambda *refs: finishing(count, columns, *refs),
        out_shape=[
            jax.ShapeDtypeStruct(factor.shape, jnp.bfloat16),
            jax.ShapeDtypeStruct((64, 64), jnp.float32),
            jax.ShapeDtypeStruct((64, 64), jnp.float32),
        ],
        compiler_params=pltpu.CompilerParams(vmem_limit_bytes=8 * MIB),
        name="finishing",
    )(got, factor)


def shards(data, w_rows, h_init):
    members = lax.axis_size("row")
    zs = members // 2
    count = lax.axis_size("col")
    columns = data.shape[1] * count
    pairs = [[2 * z + c for c in range(2)] for z in range(zs)]
    levels = [[2 * z + c for z in range(zs)] for c in range(2)]

    own, send, start = multiplied(zs, w_rows, data, h_init)
    got = lax.all_gather(send, "row", axis=0, tiled=True, axis_index_groups=pairs)
    parts = packed(zs, own, got)
    parts = lax.all_to_all(parts, "row", 0, 0, tiled=True, axis_index_groups=levels)
    copies = iterated(zs, parts, start)
    blocks = lax.all_to_all(copies, "row", 0, 0, tiled=True, axis_index_groups=levels)
    blocks = lax.all_gather(blocks, "row", axis=0, tiled=True, axis_index_groups=pairs)
    factor, terms = contracted(zs, blocks, data)
    sums = lax.all_to_all(terms.astype(jnp.float16), "col", 0, 0, tiled=True)
    return tuple(finished(count, columns, sums.astype(jnp.float32), factor))


def solution(mesh):
    in_specs = (P("row", "col"), P(None, "row"), P(None, "col"))
    out_specs = (P(None, "col"), P(), P(None, ("row", "col")))
    return jax.shard_map(shards, mesh=mesh, in_specs=in_specs, out_specs=out_specs, check_vma=False)
```

```python
import math

import jax
import jax.numpy as jnp
from jax import lax
from jax.experimental import pallas as pl
from jax.experimental.pallas import tpu as pltpu
from jax.sharding import PartitionSpec as P

ITERS = 4
LOG2E = 1.4426950408889634
LANES = 128
HALF = 64
BLOCKS = 4
STOPS = (6, 11, 14, 16)
PART = 56
CHUNK = 56
MIB = 1 << 20


def low_lanes(x):
    return lax.broadcasted_iota(jnp.int32, x.shape, 1) < HALF


def turned(x):
    return pltpu.roll(x, HALF, 1)


def stack_sides(x):
    return jnp.where(low_lanes(x[:32]), x[:32], turned(x[32:]))


def stack_copies(x):
    return jnp.where(low_lanes(x[:32]), x[:32], x[32:])


def unstack(x):
    return jnp.concatenate([x, turned(x)], axis=0)


def multiplying(zs, w_hbm, data_hbm, h_hbm, own_ref, send_ref, start_ref, data_ref, w, h, acc, sems):
    rows, columns = data_ref.shape
    width = columns // 2
    ends = [rows * part // 16 for part in STOPS]
    spans = list(zip([0, *ends], ends))
    me = lax.axis_index("row")
    core, level = lax.rem(me, 2), lax.div(me, 2)
    tile = core * (width // LANES) + lax.div(level, 2)
    copies = [
        pltpu.make_async_copy(w_hbm, w, sems.at[len(STOPS)]),
        pltpu.make_async_copy(
            h_hbm.at[:, pl.ds(pl.multiple_of(tile * LANES, LANES), LANES)], h, sems.at[len(STOPS) + 1]
        ),
    ]
    for block, (begin, end) in enumerate(spans):
        at = pl.ds(begin, end - begin)
        copies.append(pltpu.make_async_copy(data_hbm.at[at, :], data_ref.at[at, :], sems.at[block]))
    for copy in (copies[0], *copies[2:], copies[1]):
        copy.start()
    copies[0].wait()
    gram = lax.dot_general(
        w[...], jnp.concatenate([w[...], w[...]], axis=0), (((1,), (1,)), ((), ())), preferred_element_type=jnp.float32
    )
    own_ref[:, width:] = gram
    send_ref[:, width:] = gram
    for block, (begin, end) in enumerate(spans):
        copies[2 + block].wait()
        at = slice(begin, end)
        part = jnp.dot(w[:, at], data_ref[at, :], preferred_element_type=jnp.float32)
        if block == 0:
            acc[...] = part
        else:
            acc[...] += part
    first = core == 0
    left = acc[:, :width]
    right = acc[:, width:]
    own_ref[:, :width] = jnp.where(first, left, right)
    send_ref[:, :width] = jnp.where(first, right, left)
    copies[1].wait()
    begin = h[...]
    start_ref[...] = jnp.where(lax.rem(level, 2) == 0, begin, turned(begin))


def multiplied(zs, w_rows, data, h_init):
    rows, columns = data.shape
    rank = w_rows.shape[0]
    half = jax.ShapeDtypeStruct((rank, columns // 2 + LANES), jnp.float32)
    start = jax.ShapeDtypeStruct((rank, LANES), jnp.float32)
    return pl.pallas_call(
        lambda *refs: multiplying(zs, *refs),
        in_specs=[pl.BlockSpec(memory_space=pl.ANY)] * 3,
        out_specs=[pl.BlockSpec(memory_space=pltpu.VMEM)] * 3,
        out_shape=[half, half, start],
        scratch_shapes=[
            pltpu.VMEM(data.shape, data.dtype),
            pltpu.VMEM(w_rows.shape, w_rows.dtype),
            pltpu.VMEM((rank, LANES), jnp.float32),
            pltpu.VMEM((rank, columns), jnp.float32),
            pltpu.SemaphoreType.DMA((len(STOPS) + 2,)),
        ],
        compiler_params=pltpu.CompilerParams(vmem_limit_bytes=56045568),
        name="multiplying",
    )(w_rows, data, h_init)


def folded_of(outer):
    top, low = outer[:32], outer[32:]
    lane = lax.broadcasted_iota(jnp.int32, top.shape, 1)
    row = lax.broadcasted_iota(jnp.int32, top.shape, 0)
    folded = jnp.where((lane % HALF < 32) & (row > lane % 32), pltpu.roll(low, 96, 1), top)
    return jnp.where(low_lanes(folded[:16]), folded[:16], folded[16:])


def unfolded(folded, diagonal):
    upper = jnp.concatenate([folded, turned(folded)], axis=0)
    upper = jnp.concatenate([upper, pltpu.roll(upper, 32, 1)], axis=0)
    mirror = jnp.transpose(upper)[:HALF, :]
    upper = upper[:, :HALF]
    row = lax.broadcasted_iota(jnp.int32, upper.shape, 0)
    lane = lax.broadcasted_iota(jnp.int32, upper.shape, 1)
    held = ((row < 32) & (row < lane)) | ((lane >= 32) & (row > lane))
    return jnp.where(row == lane, diagonal, jnp.where(held, upper, mirror))


def packing(zs, own_ref, got_ref, out_ref):
    width = own_ref.shape[1] - LANES
    rank = own_ref.shape[0]
    theirs = pl.ds(pl.multiple_of((1 - lax.rem(lax.axis_index("row"), 2)) * rank, 8), rank)
    whole = own_ref[:, width:] + got_ref[theirs, width:]
    gram = folded_of(whole)
    row = lax.broadcasted_iota(jnp.int32, whole.shape, 0)
    lane = lax.broadcasted_iota(jnp.int32, whole.shape, 1)
    diagonal = jnp.sum(jnp.where(row == lane % HALF, whole, 0.0), axis=0, keepdims=True)
    diagonal = jnp.broadcast_to(diagonal, (8, LANES))
    for tile in range(width // LANES):
        at = slice(tile * LANES, (tile + 1) * LANES)
        x = own_ref[:, at] + got_ref[theirs, at]
        top, low = x[:32], x[32:]
        left = low_lanes(top)
        for side, block in enumerate((jnp.where(left, top, turned(low)), jnp.where(left, turned(top), low))):
            base = (2 * tile + side) * PART
            out_ref[base : base + 32, :] = block
            out_ref[base + 32 : base + 48, :] = gram
            out_ref[base + 48 : base + 56, :] = diagonal


def packed(zs, own, got):
    return pl.pallas_call(
        lambda *refs: packing(zs, *refs),
        out_shape=jax.ShapeDtypeStruct((zs * PART, LANES), jnp.float32),
        compiler_params=pltpu.CompilerParams(vmem_limit_bytes=8 * MIB),
        name="packing",
    )(own, got)


def iterating(zs, got_ref, start_ref, out_ref):
    total = got_ref[0:PART, :]
    for part in range(1, zs):
        total = total + got_ref[part * PART : part * PART + PART, :]
    gram = unfolded(total[32:48], total[48:49, :HALF])
    target = unstack(total[:32])
    lip = jnp.max(jnp.sum(gram, axis=1, keepdims=True))
    factor = start_ref[...]
    ahead = factor
    momentum = 1.0
    for step in range(ITERS):
        slope = jnp.dot(
            gram, ahead, precision=lax.Precision.HIGHEST, preferred_element_type=jnp.float32
        ) - target
        fresh = jnp.maximum(ahead - slope / lip, 0.0)
        following = (1.0 + math.sqrt(1.0 + 4.0 * momentum * momentum)) / 2.0
        ahead = fresh + (momentum - 1.0) / following * (fresh - factor)
        factor = fresh
        momentum = following
    block = stack_sides(factor)
    for part in range(zs):
        out_ref[part * 32 : part * 32 + 32, :] = block


def iterated(zs, got, start):
    return pl.pallas_call(
        lambda *refs: iterating(zs, *refs),
        out_shape=jax.ShapeDtypeStruct((zs * 32, LANES), jnp.float32),
        compiler_params=pltpu.CompilerParams(vmem_limit_bytes=8 * MIB),
        name="iterating",
    )(got, start)


def fold_masks(shape):
    row = lax.broadcasted_iota(jnp.int32, shape, 0)
    lane = lax.broadcasted_iota(jnp.int32, shape, 1)
    row = row + jnp.where(lane < HALF, 0, 16)
    return lane % HALF < 32, row > lane % 32


def contracting(zs, got_ref, data_ref, factor_ref, out_ref, lines):
    width = zs * HALF
    for side in range(2):
        for pair in range(zs // 2):
            first = (side * zs + 2 * pair) * 32
            second = first + 32
            a = got_ref[first : first + 32, :]
            b = got_ref[second : second + 32, :]
            left = low_lanes(a)
            x = jnp.concatenate([jnp.where(left, a, turned(b)), jnp.where(left, turned(a), b)], axis=0)
            at = slice(side * width + pair * LANES, side * width + (pair + 1) * LANES)
            factor_ref[:, at] = x
            low = x.astype(jnp.bfloat16)
            lines[0:64, at] = low
            lines[64:128, at] = low
    factor = factor_ref[...]
    squares = jnp.sum(factor * factor, axis=1, keepdims=True)
    both = (((1,), (1,)), ((), ()))
    outer = lax.dot_general(lines[0:64, :], lines[...], both, preferred_element_type=jnp.float32)
    ones = jnp.ones((8, lines.shape[1]), jnp.bfloat16)
    sums = lax.dot_general(ones, lines[...], both, preferred_element_type=jnp.float32)[0:1, :]
    power = jnp.ceil(jnp.log(jnp.maximum(sums, 1e-30)) * LOG2E)
    power = jnp.clip(power, -60.0, 60.0)
    most = jnp.max(power, axis=1, keepdims=True)
    shrink = jnp.exp2(-power)
    row = lax.broadcasted_iota(jnp.int32, outer.shape, 0)
    lane = lax.broadcasted_iota(jnp.int32, outer.shape, 1)
    across = jnp.sum(jnp.where(row == lane % HALF, squares, 0.0), axis=0, keepdims=True)
    across = across * shrink * shrink * 32768.0
    wide = across * 8193.0
    high = wide - (wide - across)
    line = lax.broadcasted_iota(jnp.int32, (8, LANES), 0)
    extra = jnp.where(
        line == 0,
        jnp.where(low_lanes(high), high, across - high),
        jnp.where(line == 1, power, jnp.where(line == 2, power + most, 0.0)),
    )
    outer = outer * (shrink * jnp.exp2(-most) * 32768.0)
    folded = folded_of(outer)
    shrink = shrink * 1024.0

    parts = data_ref.shape[0] // 64
    each = parts // BLOCKS
    for block in range(BLOCKS):
        at = slice(block * each * 64, (block + 1) * each * 64)
        terms = lax.dot_general(data_ref[at, :], lines[...], both, preferred_element_type=jnp.float32) * shrink
        for part in range(each):
            base = (block * each + part) * CHUNK
            out_ref[base : base + 32, :] = stack_copies(terms[part * 64 : part * 64 + 64])
            out_ref[base + 32 : base + 48, :] = folded
            out_ref[base + 48 : base + 56, :] = extra


def contracted(zs, got, data):
    rows, columns = data.shape
    return pl.pallas_call(
        lambda *refs: contracting(zs, *refs),
        out_shape=[
            jax.ShapeDtypeStruct((64, columns), jnp.float32),
            jax.ShapeDtypeStruct((rows // 64 * CHUNK, LANES), jnp.float32),
        ],
        in_specs=[pl.BlockSpec(memory_space=pltpu.VMEM)] * 2,
        out_specs=[pl.BlockSpec(memory_space=pltpu.VMEM)] * 2,
        scratch_shapes=[pltpu.VMEM((LANES, columns), jnp.bfloat16)],
        compiler_params=pltpu.CompilerParams(vmem_limit_bytes=16 * MIB),
        name="contracting",
    )(got, data)


def finishing(count, columns, got_ref, factor_ref, scaled_ref, gram_ref, terms_ref):
    folded_in, lower = fold_masks((16, LANES))
    swapped = folded_in & lower
    terms = jnp.zeros((32, LANES), jnp.float32)
    folded = jnp.zeros((16, LANES), jnp.float32)
    squares = jnp.zeros((1, LANES), jnp.float32)
    for part in range(count):
        base = part * CHUNK
        extra = got_ref[base + 48 : base + 56, :]
        grown = jnp.exp2(extra[1:3, :])
        grow, pair = grown[0:1], grown[1:2]
        terms = terms + got_ref[base : base + 32, :] * grow
        folded = folded + got_ref[base + 32 : base + 48, :] * jnp.where(swapped, pltpu.roll(pair, 96, 1), pair)
        squares = squares + (extra[0:1, :] + turned(extra[0:1, :])) * (grow * grow)
    squares = squares[:, :HALF] * (1.0 / 32768.0)
    outer = unfolded(folded * (1.0 / 32768.0), squares)
    row = lax.broadcasted_iota(jnp.int32, outer.shape, 0)
    lane = lax.broadcasted_iota(jnp.int32, outer.shape, 1)

    def scale_of(squares):
        mean = squares / columns + 1e-06
        first = lax.rsqrt(mean)
        return first * (1.5 - 0.5 * mean * first * first)

    across = scale_of(squares)
    down = scale_of(jnp.sum(jnp.where(row == lane, squares, 0.0), axis=1, keepdims=True))
    scaled_ref[...] = (factor_ref[...] * down).astype(jnp.bfloat16)
    gram_ref[...] = outer * down * across / columns
    terms = jnp.transpose(unstack(terms))[:HALF, :]
    terms_ref[...] = terms * down * (1.0 / 1024.0) / columns


def finished(count, columns, got, factor):
    return pl.pallas_call(
        lambda *refs: finishing(count, columns, *refs),
        out_shape=[
            jax.ShapeDtypeStruct(factor.shape, jnp.bfloat16),
            jax.ShapeDtypeStruct((64, 64), jnp.float32),
            jax.ShapeDtypeStruct((64, 64), jnp.float32),
        ],
        compiler_params=pltpu.CompilerParams(vmem_limit_bytes=8 * MIB),
        name="finishing",
    )(got, factor)


def shards(data, w_rows, h_init):
    members = lax.axis_size("row")
    zs = members // 2
    count = lax.axis_size("col")
    columns = data.shape[1] * count
    pairs = [[2 * z + c for c in range(2)] for z in range(zs)]
    levels = [[2 * z + c for z in range(zs)] for c in range(2)]

    own, send, start = multiplied(zs, w_rows, data, h_init)
    got = lax.all_gather(send, "row", axis=0, tiled=True, axis_index_groups=pairs)
    parts = packed(zs, own, got)
    parts = lax.all_to_all(parts, "row", 0, 0, tiled=True, axis_index_groups=levels)
    copies = iterated(zs, parts, start)
    blocks = lax.all_to_all(copies, "row", 0, 0, tiled=True, axis_index_groups=levels)
    blocks = lax.all_gather(blocks, "row", axis=0, tiled=True, axis_index_groups=pairs)
    factor, terms = contracted(zs, blocks, data)
    sums = lax.all_to_all(terms.astype(jnp.float16), "col", 0, 0, tiled=True)
    return tuple(finished(count, columns, sums.astype(jnp.float32), factor))


def solution(mesh):
    in_specs = (P("row", "col"), P(None, "row"), P(None, "col"))
    out_specs = (P(None, "col"), P(), P(None, ("row", "col")))
    return jax.shard_map(shards, mesh=mesh, in_specs=in_specs, out_specs=out_specs, check_vma=False)
```

```python
import math

import jax
import jax.numpy as jnp
from jax import lax
from jax.experimental import pallas as pl
from jax.experimental.pallas import tpu as pltpu
from jax.sharding import PartitionSpec as P

ITERS = 4
LOG2E = 1.4426950408889634
LANES = 128
HALF = 64
BLOCKS = 4
STOPS = (6, 11, 14, 16)
PART = 56
CHUNK = 56
MIB = 1 << 20


def low_lanes(x):
    return lax.broadcasted_iota(jnp.int32, x.shape, 1) < HALF


def turned(x):
    return pltpu.roll(x, HALF, 1)


def stack_sides(x):
    return jnp.where(low_lanes(x[:32]), x[:32], turned(x[32:]))


def stack_copies(x):
    return jnp.where(low_lanes(x[:32]), x[:32], x[32:])


def unstack(x):
    return jnp.concatenate([x, turned(x)], axis=0)


def multiplying(zs, w_hbm, data_hbm, h_hbm, own_ref, send_ref, start_ref, data_ref, w, h, acc, sems):
    rows, columns = data_ref.shape
    width = columns // 2
    ends = [rows * part // 16 for part in STOPS]
    spans = list(zip([0, *ends], ends))
    me = lax.axis_index("row")
    core, level = lax.rem(me, 2), lax.div(me, 2)
    tile = core * (width // LANES) + lax.div(level, 2)
    copies = [
        pltpu.make_async_copy(w_hbm, w, sems.at[len(STOPS)]),
        pltpu.make_async_copy(
            h_hbm.at[:, pl.ds(pl.multiple_of(tile * LANES, LANES), LANES)], h, sems.at[len(STOPS) + 1]
        ),
    ]
    for block, (begin, end) in enumerate(spans):
        at = pl.ds(begin, end - begin)
        copies.append(pltpu.make_async_copy(data_hbm.at[at, :], data_ref.at[at, :], sems.at[block]))
    for copy in (copies[0], *copies[2:], copies[1]):
        copy.start()
    copies[0].wait()
    gram = lax.dot_general(
        w[...], jnp.concatenate([w[...], w[...]], axis=0), (((1,), (1,)), ((), ())), preferred_element_type=jnp.float32
    )
    own_ref[:, width:] = gram
    send_ref[:, width:] = gram
    for block, (begin, end) in enumerate(spans):
        copies[2 + block].wait()
        at = slice(begin, end)
        part = jnp.dot(w[:, at], data_ref[at, :], preferred_element_type=jnp.float32)
        if block == 0:
            acc[...] = part
        else:
            acc[...] += part
    first = core == 0
    left = acc[:, :width]
    right = acc[:, width:]
    own_ref[:, :width] = jnp.where(first, left, right)
    send_ref[:, :width] = jnp.where(first, right, left)
    copies[1].wait()
    begin = h[...]
    start_ref[...] = jnp.where(lax.rem(level, 2) == 0, begin, turned(begin))


def multiplied(zs, w_rows, data, h_init):
    rows, columns = data.shape
    rank = w_rows.shape[0]
    half = jax.ShapeDtypeStruct((rank, columns // 2 + LANES), jnp.float32)
    start = jax.ShapeDtypeStruct((rank, LANES), jnp.float32)
    return pl.pallas_call(
        lambda *refs: multiplying(zs, *refs),
        in_specs=[pl.BlockSpec(memory_space=pl.ANY)] * 3,
        out_specs=[pl.BlockSpec(memory_space=pltpu.VMEM)] * 3,
        out_shape=[half, half, start],
        scratch_shapes=[
            pltpu.VMEM(data.shape, data.dtype),
            pltpu.VMEM(w_rows.shape, w_rows.dtype),
            pltpu.VMEM((rank, LANES), jnp.float32),
            pltpu.VMEM((rank, columns), jnp.float32),
            pltpu.SemaphoreType.DMA((len(STOPS) + 2,)),
        ],
        compiler_params=pltpu.CompilerParams(vmem_limit_bytes=56045568),
        name="multiplying",
    )(w_rows, data, h_init)


def folded_of(outer):
    top, low = outer[:32], outer[32:]
    lane = lax.broadcasted_iota(jnp.int32, top.shape, 1)
    row = lax.broadcasted_iota(jnp.int32, top.shape, 0)
    folded = jnp.where((lane % HALF < 32) & (row > lane % 32), pltpu.roll(low, 96, 1), top)
    return jnp.where(low_lanes(folded[:16]), folded[:16], folded[16:])


def unfolded(folded, diagonal):
    upper = jnp.concatenate([folded, turned(folded)], axis=0)
    upper = jnp.concatenate([upper, pltpu.roll(upper, 32, 1)], axis=0)
    mirror = jnp.transpose(upper)[:HALF, :]
    upper = upper[:, :HALF]
    row = lax.broadcasted_iota(jnp.int32, upper.shape, 0)
    lane = lax.broadcasted_iota(jnp.int32, upper.shape, 1)
    held = ((row < 32) & (row < lane)) | ((lane >= 32) & (row > lane))
    return jnp.where(row == lane, diagonal, jnp.where(held, upper, mirror))


def packing(zs, own_ref, got_ref, out_ref):
    width = own_ref.shape[1] - LANES
    rank = own_ref.shape[0]
    theirs = pl.ds(pl.multiple_of((1 - lax.rem(lax.axis_index("row"), 2)) * rank, 8), rank)
    whole = own_ref[:, width:] + got_ref[theirs, width:]
    gram = folded_of(whole)
    row = lax.broadcasted_iota(jnp.int32, whole.shape, 0)
    lane = lax.broadcasted_iota(jnp.int32, whole.shape, 1)
    diagonal = jnp.sum(jnp.where(row == lane % HALF, whole, 0.0), axis=0, keepdims=True)
    diagonal = jnp.broadcast_to(diagonal, (8, LANES))
    for tile in range(width // LANES):
        at = slice(tile * LANES, (tile + 1) * LANES)
        x = own_ref[:, at] + got_ref[theirs, at]
        top, low = x[:32], x[32:]
        left = low_lanes(top)
        for side, block in enumerate((jnp.where(left, top, turned(low)), jnp.where(left, turned(top), low))):
            base = (2 * tile + side) * PART
            out_ref[base : base + 32, :] = block
            out_ref[base + 32 : base + 48, :] = gram
            out_ref[base + 48 : base + 56, :] = diagonal


def packed(zs, own, got):
    return pl.pallas_call(
        lambda *refs: packing(zs, *refs),
        out_shape=jax.ShapeDtypeStruct((zs * PART, LANES), jnp.float32),
        compiler_params=pltpu.CompilerParams(vmem_limit_bytes=8 * MIB),
        name="packing",
    )(own, got)


def iterating(zs, got_ref, start_ref, out_ref):
    total = got_ref[0:PART, :]
    for part in range(1, zs):
        total = total + got_ref[part * PART : part * PART + PART, :]
    gram = unfolded(total[32:48], total[48:49, :HALF])
    target = unstack(total[:32])
    lip = jnp.max(jnp.sum(gram, axis=1, keepdims=True))
    factor = start_ref[...]
    ahead = factor
    momentum = 1.0
    for step in range(ITERS):
        slope = jnp.dot(
            gram, ahead, precision=lax.Precision.HIGHEST, preferred_element_type=jnp.float32
        ) - target
        fresh = jnp.maximum(ahead - slope / lip, 0.0)
        following = (1.0 + math.sqrt(1.0 + 4.0 * momentum * momentum)) / 2.0
        ahead = fresh + (momentum - 1.0) / following * (fresh - factor)
        factor = fresh
        momentum = following
    block = stack_sides(factor)
    for part in range(zs):
        out_ref[part * 32 : part * 32 + 32, :] = block


def iterated(zs, got, start):
    return pl.pallas_call(
        lambda *refs: iterating(zs, *refs),
        out_shape=jax.ShapeDtypeStruct((zs * 32, LANES), jnp.float32),
        compiler_params=pltpu.CompilerParams(vmem_limit_bytes=8 * MIB),
        name="iterating",
    )(got, start)


def fold_masks(shape):
    row = lax.broadcasted_iota(jnp.int32, shape, 0)
    lane = lax.broadcasted_iota(jnp.int32, shape, 1)
    row = row + jnp.where(lane < HALF, 0, 16)
    return lane % HALF < 32, row > lane % 32


def contracting(zs, got_ref, data_ref, factor_ref, out_ref, lines):
    width = zs * HALF
    for side in range(2):
        for pair in range(zs // 2):
            first = (side * zs + 2 * pair) * 32
            second = first + 32
            a = got_ref[first : first + 32, :]
            b = got_ref[second : second + 32, :]
            left = low_lanes(a)
            x = jnp.concatenate([jnp.where(left, a, turned(b)), jnp.where(left, turned(a), b)], axis=0)
            at = slice(side * width + pair * LANES, side * width + (pair + 1) * LANES)
            factor_ref[:, at] = x
            low = x.astype(jnp.bfloat16)
            lines[0:64, at] = low
            lines[64:128, at] = low
    factor = factor_ref[...]
    squares = jnp.sum(factor * factor, axis=1, keepdims=True)
    both = (((1,), (1,)), ((), ()))
    outer = lax.dot_general(lines[0:64, :], lines[...], both, preferred_element_type=jnp.float32)
    ones = jnp.ones((8, lines.shape[1]), jnp.bfloat16)
    sums = lax.dot_general(ones, lines[...], both, preferred_element_type=jnp.float32)[0:1, :]
    power = jnp.ceil(jnp.log(jnp.maximum(sums, 1e-30)) * LOG2E)
    power = jnp.clip(power, -40.0, 60.0)
    most = jnp.max(power, axis=1, keepdims=True)
    shrink = jnp.exp2(-power)
    row = lax.broadcasted_iota(jnp.int32, outer.shape, 0)
    lane = lax.broadcasted_iota(jnp.int32, outer.shape, 1)
    across = jnp.sum(jnp.where(row == lane % HALF, squares, 0.0), axis=0, keepdims=True)
    across = across * shrink * shrink * 32768.0
    wide = across * 8193.0
    high = wide - (wide - across)
    line = lax.broadcasted_iota(jnp.int32, (8, LANES), 0)
    extra = jnp.where(
        line == 0,
        jnp.where(low_lanes(high), high, across - high),
        jnp.where(line == 1, power, jnp.where(line == 2, power + most, 0.0)),
    )
    outer = (outer * shrink) * (jnp.exp2(-most) * 32768.0)
    folded = folded_of(outer)
    shrink = shrink * 1024.0

    parts = data_ref.shape[0] // 64
    each = parts // BLOCKS
    for block in range(BLOCKS):
        at = slice(block * each * 64, (block + 1) * each * 64)
        terms = lax.dot_general(data_ref[at, :], lines[...], both, preferred_element_type=jnp.float32) * shrink
        for part in range(each):
            base = (block * each + part) * CHUNK
            out_ref[base : base + 32, :] = stack_copies(terms[part * 64 : part * 64 + 64])
            out_ref[base + 32 : base + 48, :] = folded
            out_ref[base + 48 : base + 56, :] = extra


def contracted(zs, got, data):
    rows, columns = data.shape
    return pl.pallas_call(
        lambda *refs: contracting(zs, *refs),
        out_shape=[
            jax.ShapeDtypeStruct((64, columns), jnp.float32),
            jax.ShapeDtypeStruct((rows // 64 * CHUNK, LANES), jnp.float32),
        ],
        in_specs=[pl.BlockSpec(memory_space=pltpu.VMEM)] * 2,
        out_specs=[pl.BlockSpec(memory_space=pltpu.VMEM)] * 2,
        scratch_shapes=[pltpu.VMEM((LANES, columns), jnp.bfloat16)],
        compiler_params=pltpu.CompilerParams(vmem_limit_bytes=16 * MIB),
        name="contracting",
    )(got, data)


def finishing(count, columns, got_ref, factor_ref, scaled_ref, gram_ref, terms_ref):
    folded_in, lower = fold_masks((16, LANES))
    swapped = folded_in & lower
    terms = jnp.zeros((32, LANES), jnp.float32)
    folded = jnp.zeros((16, LANES), jnp.float32)
    squares = jnp.zeros((1, LANES), jnp.float32)
    for part in range(count):
        base = part * CHUNK
        extra = got_ref[base + 48 : base + 56, :]
        grown = jnp.exp2(extra[1:3, :])
        grow, pair = grown[0:1], grown[1:2]
        terms = terms + got_ref[base : base + 32, :] * grow
        folded = folded + got_ref[base + 32 : base + 48, :] * jnp.where(swapped, pltpu.roll(pair, 96, 1), pair)
        squares = squares + (extra[0:1, :] + turned(extra[0:1, :])) * (grow * grow)
    squares = squares[:, :HALF] * (1.0 / 32768.0)
    outer = unfolded(folded * (1.0 / 32768.0), squares)
    row = lax.broadcasted_iota(jnp.int32, outer.shape, 0)
    lane = lax.broadcasted_iota(jnp.int32, outer.shape, 1)

    def scale_of(squares):
        mean = squares / columns + 1e-06
        first = lax.rsqrt(mean)
        return first * (1.5 - 0.5 * mean * first * first)

    across = scale_of(squares)
    down = scale_of(jnp.sum(jnp.where(row == lane, squares, 0.0), axis=1, keepdims=True))
    scaled_ref[...] = (factor_ref[...] * down).astype(jnp.bfloat16)
    gram_ref[...] = outer * down * across / columns
    terms = jnp.transpose(unstack(terms))[:HALF, :]
    terms_ref[...] = terms * down * (1.0 / 1024.0) / columns


def finished(count, columns, got, factor):
    return pl.pallas_call(
        lambda *refs: finishing(count, columns, *refs),
        out_shape=[
            jax.ShapeDtypeStruct(factor.shape, jnp.bfloat16),
            jax.ShapeDtypeStruct((64, 64), jnp.float32),
            jax.ShapeDtypeStruct((64, 64), jnp.float32),
        ],
        compiler_params=pltpu.CompilerParams(vmem_limit_bytes=8 * MIB),
        name="finishing",
    )(got, factor)


def shards(data, w_rows, h_init):
    members = lax.axis_size("row")
    zs = members // 2
    count = lax.axis_size("col")
    columns = data.shape[1] * count
    pairs = [[2 * z + c for c in range(2)] for z in range(zs)]
    levels = [[2 * z + c for z in range(zs)] for c in range(2)]

    own, send, start = multiplied(zs, w_rows, data, h_init)
    got = lax.all_gather(send, "row", axis=0, tiled=True, axis_index_groups=pairs)
    parts = packed(zs, own, got)
    parts = lax.all_to_all(parts, "row", 0, 0, tiled=True, axis_index_groups=levels)
    copies = iterated(zs, parts, start)
    blocks = lax.all_to_all(copies, "row", 0, 0, tiled=True, axis_index_groups=levels)
    blocks = lax.all_gather(blocks, "row", axis=0, tiled=True, axis_index_groups=pairs)
    factor, terms = contracted(zs, blocks, data)
    sums = lax.all_to_all(terms.astype(jnp.float16), "col", 0, 0, tiled=True)
    return tuple(finished(count, columns, sums.astype(jnp.float32), factor))


def solution(mesh):
    in_specs = (P("row", "col"), P(None, "row"), P(None, "col"))
    out_specs = (P(None, "col"), P(), P(None, ("row", "col")))
    return jax.shard_map(shards, mesh=mesh, in_specs=in_specs, out_specs=out_specs, check_vma=False)
```

```python
import math

import jax
import jax.numpy as jnp
from jax import lax
from jax.experimental import pallas as pl
from jax.experimental.pallas import tpu as pltpu
from jax.sharding import PartitionSpec as P

ITERS = 4
LOG2E = 1.4426950408889634
LANES = 128
HALF = 64
BLOCKS = 4
STOPS = (6, 11, 14, 16)
PART = 56
CHUNK = 56
MIB = 1 << 20


def low_lanes(x):
    return lax.broadcasted_iota(jnp.int32, x.shape, 1) < HALF


def turned(x):
    return pltpu.roll(x, HALF, 1)


def stack_sides(x):
    return jnp.where(low_lanes(x[:32]), x[:32], turned(x[32:]))


def stack_copies(x):
    return jnp.where(low_lanes(x[:32]), x[:32], x[32:])


def unstack(x):
    return jnp.concatenate([x, turned(x)], axis=0)


def multiplying(zs, w_hbm, data_hbm, h_hbm, own_ref, send_ref, start_ref, data_ref, w, h, acc, sems):
    rows, columns = data_ref.shape
    width = columns // 2
    ends = [rows * part // 16 for part in STOPS]
    spans = list(zip([0, *ends], ends))
    me = lax.axis_index("row")
    core, level = lax.rem(me, 2), lax.div(me, 2)
    tile = core * (width // LANES) + lax.div(level, 2)
    copies = [
        pltpu.make_async_copy(w_hbm, w, sems.at[len(STOPS)]),
        pltpu.make_async_copy(
            h_hbm.at[:, pl.ds(pl.multiple_of(tile * LANES, LANES), LANES)], h, sems.at[len(STOPS) + 1]
        ),
    ]
    for block, (begin, end) in enumerate(spans):
        at = pl.ds(begin, end - begin)
        copies.append(pltpu.make_async_copy(data_hbm.at[at, :], data_ref.at[at, :], sems.at[block]))
    for copy in (copies[0], *copies[2:], copies[1]):
        copy.start()
    copies[0].wait()
    gram = lax.dot_general(
        w[...], jnp.concatenate([w[...], w[...]], axis=0), (((1,), (1,)), ((), ())), preferred_element_type=jnp.float32
    )
    own_ref[:, width:] = gram
    send_ref[:, width:] = gram
    for block, (begin, end) in enumerate(spans):
        copies[2 + block].wait()
        at = slice(begin, end)
        part = jnp.dot(w[:, at], data_ref[at, :], preferred_element_type=jnp.float32)
        if block == 0:
            acc[...] = part
        else:
            acc[...] += part
    first = core == 0
    left = acc[:, :width]
    right = acc[:, width:]
    own_ref[:, :width] = jnp.where(first, left, right)
    send_ref[:, :width] = jnp.where(first, right, left)
    copies[1].wait()
    begin = h[...]
    start_ref[...] = jnp.where(lax.rem(level, 2) == 0, begin, turned(begin))


def multiplied(zs, w_rows, data, h_init):
    rows, columns = data.shape
    rank = w_rows.shape[0]
    half = jax.ShapeDtypeStruct((rank, columns // 2 + LANES), jnp.float32)
    start = jax.ShapeDtypeStruct((rank, LANES), jnp.float32)
    return pl.pallas_call(
        lambda *refs: multiplying(zs, *refs),
        in_specs=[pl.BlockSpec(memory_space=pl.ANY)] * 3,
        out_specs=[pl.BlockSpec(memory_space=pltpu.VMEM)] * 3,
        out_shape=[half, half, start],
        scratch_shapes=[
            pltpu.VMEM(data.shape, data.dtype),
            pltpu.VMEM(w_rows.shape, w_rows.dtype),
            pltpu.VMEM((rank, LANES), jnp.float32),
            pltpu.VMEM((rank, columns), jnp.float32),
            pltpu.SemaphoreType.DMA((len(STOPS) + 2,)),
        ],
        compiler_params=pltpu.CompilerParams(vmem_limit_bytes=56045568),
        name="multiplying",
    )(w_rows, data, h_init)


def folded_of(outer):
    top, low = outer[:32], outer[32:]
    lane = lax.broadcasted_iota(jnp.int32, top.shape, 1)
    row = lax.broadcasted_iota(jnp.int32, top.shape, 0)
    folded = jnp.where((lane % HALF < 32) & (row > lane % 32), pltpu.roll(low, 96, 1), top)
    return jnp.where(low_lanes(folded[:16]), folded[:16], folded[16:])


def unfolded(folded, diagonal):
    upper = jnp.concatenate([folded, turned(folded)], axis=0)
    upper = jnp.concatenate([upper, pltpu.roll(upper, 32, 1)], axis=0)
    mirror = jnp.transpose(upper)[:HALF, :]
    upper = upper[:, :HALF]
    row = lax.broadcasted_iota(jnp.int32, upper.shape, 0)
    lane = lax.broadcasted_iota(jnp.int32, upper.shape, 1)
    held = ((row < 32) & (row < lane)) | ((lane >= 32) & (row > lane))
    return jnp.where(row == lane, diagonal, jnp.where(held, upper, mirror))


def packing(zs, own_ref, got_ref, out_ref):
    width = own_ref.shape[1] - LANES
    rank = own_ref.shape[0]
    theirs = pl.ds(pl.multiple_of((1 - lax.rem(lax.axis_index("row"), 2)) * rank, 8), rank)
    whole = own_ref[:, width:] + got_ref[theirs, width:]
    gram = folded_of(whole)
    row = lax.broadcasted_iota(jnp.int32, whole.shape, 0)
    lane = lax.broadcasted_iota(jnp.int32, whole.shape, 1)
    diagonal = jnp.sum(jnp.where(row == lane % HALF, whole, 0.0), axis=0, keepdims=True)
    diagonal = jnp.broadcast_to(diagonal, (8, LANES))
    for tile in range(width // LANES):
        at = slice(tile * LANES, (tile + 1) * LANES)
        x = own_ref[:, at] + got_ref[theirs, at]
        top, low = x[:32], x[32:]
        left = low_lanes(top)
        for side, block in enumerate((jnp.where(left, top, turned(low)), jnp.where(left, turned(top), low))):
            base = (2 * tile + side) * PART
            out_ref[base : base + 32, :] = block
            out_ref[base + 32 : base + 48, :] = gram
            out_ref[base + 48 : base + 56, :] = diagonal


def packed(zs, own, got):
    return pl.pallas_call(
        lambda *refs: packing(zs, *refs),
        out_shape=jax.ShapeDtypeStruct((zs * PART, LANES), jnp.float32),
        compiler_params=pltpu.CompilerParams(vmem_limit_bytes=8 * MIB),
        name="packing",
    )(own, got)


def split(x):
    one = x.astype(jnp.bfloat16)
    rest = x - one.astype(jnp.float32)
    two = rest.astype(jnp.bfloat16)
    three = (rest - two.astype(jnp.float32)).astype(jnp.bfloat16)
    return one, two, three


def iterating(zs, got_ref, start_ref, out_ref):
    total = got_ref[0:PART, :]
    for part in range(1, zs):
        total = total + got_ref[part * PART : part * PART + PART, :]
    gram = unfolded(total[32:48], total[48:49, :HALF])
    target = unstack(total[:32])
    inverse = 1.0 / jnp.max(jnp.sum(gram, axis=0, keepdims=True))
    one, two, three = split(gram)
    left = jnp.concatenate([one, one, two, one, two, three], axis=1)
    factor = start_ref[...]
    ahead = factor
    momentum = 1.0
    for step in range(ITERS):
        one, two, three = split(ahead)
        right = jnp.concatenate([one, two, one, three, two, one], axis=0)
        slope = jnp.dot(left, right, preferred_element_type=jnp.float32) - target
        fresh = jnp.maximum(ahead - slope * inverse, 0.0)
        following = (1.0 + math.sqrt(1.0 + 4.0 * momentum * momentum)) / 2.0
        ahead = fresh + (momentum - 1.0) / following * (fresh - factor)
        factor = fresh
        momentum = following
    block = stack_sides(factor)
    for part in range(zs):
        out_ref[part * 32 : part * 32 + 32, :] = block


def iterated(zs, got, start):
    return pl.pallas_call(
        lambda *refs: iterating(zs, *refs),
        out_shape=jax.ShapeDtypeStruct((zs * 32, LANES), jnp.float32),
        compiler_params=pltpu.CompilerParams(vmem_limit_bytes=8 * MIB),
        name="iterating",
    )(got, start)


def fold_masks(shape):
    row = lax.broadcasted_iota(jnp.int32, shape, 0)
    lane = lax.broadcasted_iota(jnp.int32, shape, 1)
    row = row + jnp.where(lane < HALF, 0, 16)
    return lane % HALF < 32, row > lane % 32


def contracting(zs, got_ref, data_ref, factor_ref, out_ref, lines):
    width = zs * HALF
    for side in range(2):
        for pair in range(zs // 2):
            first = (side * zs + 2 * pair) * 32
            second = first + 32
            a = got_ref[first : first + 32, :]
            b = got_ref[second : second + 32, :]
            left = low_lanes(a)
            x = jnp.concatenate([jnp.where(left, a, turned(b)), jnp.where(left, turned(a), b)], axis=0)
            at = slice(side * width + pair * LANES, side * width + (pair + 1) * LANES)
            factor_ref[:, at] = x
            low = x.astype(jnp.bfloat16)
            lines[0:64, at] = low
            lines[64:128, at] = low
    factor = factor_ref[...]
    squares = jnp.sum(factor * factor, axis=1, keepdims=True)
    both = (((1,), (1,)), ((), ()))
    outer = lax.dot_general(lines[0:64, :], lines[...], both, preferred_element_type=jnp.float32)
    ones = jnp.ones((8, lines.shape[1]), jnp.bfloat16)
    sums = lax.dot_general(ones, lines[...], both, preferred_element_type=jnp.float32)[0:1, :]
    power = jnp.ceil(jnp.log(jnp.maximum(sums, 1e-30)) * LOG2E)
    power = jnp.clip(power, -40.0, 60.0)
    most = jnp.max(power, axis=1, keepdims=True)
    shrink = jnp.exp2(-power)
    row = lax.broadcasted_iota(jnp.int32, outer.shape, 0)
    lane = lax.broadcasted_iota(jnp.int32, outer.shape, 1)
    across = jnp.sum(jnp.where(row == lane % HALF, squares, 0.0), axis=0, keepdims=True)
    across = across * shrink * shrink * 32768.0
    wide = across * 8193.0
    high = wide - (wide - across)
    line = lax.broadcasted_iota(jnp.int32, (8, LANES), 0)
    extra = jnp.where(
        line == 0,
        jnp.where(low_lanes(high), high, across - high),
        jnp.where(line == 1, power, jnp.where(line == 2, power + most, 0.0)),
    )
    outer = (outer * shrink) * (jnp.exp2(-most) * 32768.0)
    folded = folded_of(outer)
    shrink = shrink * 1024.0

    parts = data_ref.shape[0] // 64
    each = parts // BLOCKS
    for block in range(BLOCKS):
        at = slice(block * each * 64, (block + 1) * each * 64)
        terms = lax.dot_general(data_ref[at, :], lines[...], both, preferred_element_type=jnp.float32) * shrink
        for part in range(each):
            base = (block * each + part) * CHUNK
            out_ref[base : base + 32, :] = stack_copies(terms[part * 64 : part * 64 + 64])
            out_ref[base + 32 : base + 48, :] = folded
            out_ref[base + 48 : base + 56, :] = extra


def contracted(zs, got, data):
    rows, columns = data.shape
    return pl.pallas_call(
        lambda *refs: contracting(zs, *refs),
        out_shape=[
            jax.ShapeDtypeStruct((64, columns), jnp.float32),
            jax.ShapeDtypeStruct((rows // 64 * CHUNK, LANES), jnp.float32),
        ],
        in_specs=[pl.BlockSpec(memory_space=pltpu.VMEM)] * 2,
        out_specs=[pl.BlockSpec(memory_space=pltpu.VMEM)] * 2,
        scratch_shapes=[pltpu.VMEM((LANES, columns), jnp.bfloat16)],
        compiler_params=pltpu.CompilerParams(vmem_limit_bytes=16 * MIB),
        name="contracting",
    )(got, data)


def finishing(count, columns, got_ref, factor_ref, scaled_ref, gram_ref, terms_ref):
    folded_in, lower = fold_masks((16, LANES))
    swapped = folded_in & lower
    terms = jnp.zeros((32, LANES), jnp.float32)
    folded = jnp.zeros((16, LANES), jnp.float32)
    squares = jnp.zeros((1, LANES), jnp.float32)
    for part in range(count):
        base = part * CHUNK
        extra = got_ref[base + 48 : base + 56, :]
        grown = jnp.exp2(extra[1:3, :])
        grow, pair = grown[0:1], grown[1:2]
        terms = terms + got_ref[base : base + 32, :] * grow
        folded = folded + got_ref[base + 32 : base + 48, :] * jnp.where(swapped, pltpu.roll(pair, 96, 1), pair)
        squares = squares + (extra[0:1, :] + turned(extra[0:1, :])) * (grow * grow)
    squares = squares[:, :HALF] * (1.0 / 32768.0)
    outer = unfolded(folded * (1.0 / 32768.0), squares)
    row = lax.broadcasted_iota(jnp.int32, outer.shape, 0)
    lane = lax.broadcasted_iota(jnp.int32, outer.shape, 1)

    def scale_of(squares):
        mean = squares / columns + 1e-06
        first = lax.rsqrt(mean)
        return first * (1.5 - 0.5 * mean * first * first)

    across = scale_of(squares)
    down = scale_of(jnp.sum(jnp.where(row == lane, squares, 0.0), axis=1, keepdims=True))
    scaled_ref[...] = (factor_ref[...] * down).astype(jnp.bfloat16)
    gram_ref[...] = outer * down * across / columns
    terms = jnp.transpose(unstack(terms))[:HALF, :]
    terms_ref[...] = terms * down * (1.0 / 1024.0) / columns


def finished(count, columns, got, factor):
    return pl.pallas_call(
        lambda *refs: finishing(count, columns, *refs),
        out_shape=[
            jax.ShapeDtypeStruct(factor.shape, jnp.bfloat16),
            jax.ShapeDtypeStruct((64, 64), jnp.float32),
            jax.ShapeDtypeStruct((64, 64), jnp.float32),
        ],
        compiler_params=pltpu.CompilerParams(vmem_limit_bytes=8 * MIB),
        name="finishing",
    )(got, factor)


def shards(data, w_rows, h_init):
    members = lax.axis_size("row")
    zs = members // 2
    count = lax.axis_size("col")
    columns = data.shape[1] * count
    pairs = [[2 * z + c for c in range(2)] for z in range(zs)]
    levels = [[2 * z + c for z in range(zs)] for c in range(2)]

    own, send, start = multiplied(zs, w_rows, data, h_init)
    got = lax.all_gather(send, "row", axis=0, tiled=True, axis_index_groups=pairs)
    parts = packed(zs, own, got)
    parts = lax.all_to_all(parts, "row", 0, 0, tiled=True, axis_index_groups=levels)
    copies = iterated(zs, parts, start)
    blocks = lax.all_to_all(copies, "row", 0, 0, tiled=True, axis_index_groups=levels)
    blocks = lax.all_gather(blocks, "row", axis=0, tiled=True, axis_index_groups=pairs)
    factor, terms = contracted(zs, blocks, data)
    sums = lax.all_to_all(terms.astype(jnp.float16), "col", 0, 0, tiled=True)
    return tuple(finished(count, columns, sums.astype(jnp.float32), factor))


def solution(mesh):
    in_specs = (P("row", "col"), P(None, "row"), P(None, "col"))
    out_specs = (P(None, "col"), P(), P(None, ("row", "col")))
    return jax.shard_map(shards, mesh=mesh, in_specs=in_specs, out_specs=out_specs, check_vma=False)
```
